32 devices in a mesh: rep: 1 (over z), dp: 32 (over x, y, core).
Axes of the slice: x: 4, y: 4, z: 1, core: 2. Of those that a mesh axis runs over, the one named last changes fastest.
The devices are a block of a 4x4x8 slice.
Arguments:
- g_w_gate: bfloat16 [32, 2, 768, 3072], P(('rep', 'dp'))
- g_w_up: bfloat16 [32, 2, 768, 3072], P(('rep', 'dp'))
- g_w_down: bfloat16 [32, 2, 3072, 768], P(('rep', 'dp'))
- w_gate: bfloat16 [2, 768, 3072], replicated
- w_up: bfloat16 [2, 768, 3072], replicated
- w_down: bfloat16 [2, 3072, 768], replicated
- m_w_gate: float32 [2, 768, 3072], P(None, 'dp')
- m_w_up: float32 [2, 768, 3072], P(None, 'dp')
- m_w_down: float32 [2, 3072, 768], P(None, 'dp')
- v_w_gate: float32 [2, 768, 3072], P(None, 'dp')
- v_w_up: float32 [2, 768, 3072], P(None, 'dp')
- v_w_down: float32 [2, 3072, 768], P(None, 'dp')
Outputs:
- output 1: bfloat16 [2, 768, 3072], P('rep')
- output 2: bfloat16 [2, 768, 3072], P('rep')
- output 3: bfloat16 [2, 3072, 768], P('rep')
- output 4: float32 [2, 768, 3072], P('rep', 'dp')
- output 5: float32 [2, 768, 3072], P('rep', 'dp')
- output 6: float32 [2, 3072, 768], P('rep', 'dp')
- output 7: float32 [2, 768, 3072], P('rep', 'dp')
- output 8: float32 [2, 768, 3072], P('rep', 'dp')
- output 9: float32 [2, 3072, 768], P('rep', 'dp')
All inputs are finite; a program needn't handle non-finite values.
Results may differ from the reference program's by a relative error of at most 0.022.
Values are sent between devices in bfloat16 or wider.
A program may use at most 768 MiB of HBM per device.

```python
import jax
import jax.numpy as jnp
from jax import lax

DEVICES = 32
D = 768
FF = 3072
LAYERS = 2
NAMES = ("w_gate", "w_up", "w_down")
SHAPES = {"w_gate": (LAYERS, D, FF), "w_up": (LAYERS, D, FF), "w_down": (LAYERS, FF, D)}


def setup_inputs(seed: int = 0, part: int = 0) -> dict:
    kz, *keys = jax.random.split(jax.random.key(seed), 1 + 5 * len(NAMES))
    loud = 2.0 ** jax.random.uniform(kz, (), jnp.float32, -1.0, 1.0)
    drawn = {}
    for name, key, both in zip(NAMES, keys[:3], keys[3:6], strict=True):
        own = jax.random.normal(jax.random.fold_in(key, part), (DEVICES, *SHAPES[name]), jnp.float32)
        shared = jax.random.normal(jax.random.fold_in(both, part), SHAPES[name], jnp.float32)
        drawn["g_" + name] = (loud * (0.7 * shared / DEVICES + 0.7 * own * DEVICES**-0.5)).astype(jnp.bfloat16)
    for name, key in zip(NAMES, keys[6:9], strict=True):
        drawn[name] = (jax.random.normal(key, SHAPES[name], jnp.float32) * SHAPES[name][1] ** -0.5).astype(jnp.bfloat16)
    for name, key in zip(NAMES, keys[9:12], strict=True):
        drawn["m_" + name] = loud * 0.5 * jax.random.normal(key, SHAPES[name], jnp.float32)
    for name, key in zip(NAMES, keys[12:15], strict=True):
        drawn["v_" + name] = loud * loud * jax.random.uniform(key, SHAPES[name], jnp.float32, 0.5, 1.5)
    return drawn


def adamw(w, m, v, g):
    m = 0.9 * m + 0.1 * g
    v = 0.95 * v + 0.05 * g * g
    step = m * lax.rsqrt(v + 1e-8) + 0.1 * w
    return (w - 0.02 * step).astype(jnp.bfloat16), m, v


def clipped(gradients, sum_of_squares, count):
    factor = jnp.minimum(1.0, 0.5 * lax.rsqrt(sum_of_squares / count + 1e-30))
    return [g * factor for g in gradients]


def reference(g_w_gate, g_w_up, g_w_down, w_gate, w_up, w_down, m_w_gate, m_w_up, m_w_down, v_w_gate, v_w_up, v_w_down):
    def total(terms):
        return lax.scan(lambda so_far, term: (so_far + term.astype(jnp.float32), None), jnp.zeros(terms.shape[1:], jnp.float32), terms)[0]

    gradients = [total(terms).astype(jnp.bfloat16).astype(jnp.float32) for terms in (g_w_gate, g_w_up, g_w_down)]
    gradients = clipped(gradients, sum(jnp.sum(g * g) for g in gradients), sum(g.size for g in gradients))
    new = [
        adamw(w.astype(jnp.float32), m, v, g)
        for w, m, v, g in zip((w_gate, w_up, w_down), (m_w_gate, m_w_up, m_w_down), (v_w_gate, v_w_up, v_w_down), gradients, strict=True)
    ]
    return tuple(one[which] for which in range(3) for one in new)
```

```python
import functools
import math

import jax
import jax.numpy as jnp
from jax import lax
from jax.experimental import pallas as pl
from jax.experimental.pallas import tpu as pltpu
from jax.sharding import PartitionSpec as P

LANES = 128
TILE = 8
CORES = 2
AXES = 2
HALVES = 2
QUARTERS = AXES * HALVES
F32, BF16 = jnp.float32, jnp.bfloat16


def tiled(a, *blocks):
    layers, rows, columns = a.shape
    a = a.reshape(layers, rows // TILE, TILE, columns // LANES, LANES).transpose(0, 1, 3, 2, 4)
    return a.reshape(layers, *blocks, rows * columns // (LANES * math.prod(blocks)), LANES)


def untiled(a, shape):
    layers, rows, columns = shape
    a = a.reshape(layers, rows // TILE, columns // LANES, TILE, LANES).transpose(0, 1, 3, 2, 4)
    return a.reshape(shape)


def steps(count, body):
    def run(i, carry):
        body(i)
        return carry

    lax.fori_loop(0, count, run, 0)


def exchange_kernel(n, side, *refs):
    g_refs, w_refs, m_refs, v_refs = (refs[i : i + 3] for i in (0, 3, 6, 9))
    whole, moments = refs[12:14]
    (land1, land2, grads, w_own, m_own, v_own, squares) = refs[14:21]
    (load_sem, swap_send, swap_recv, send1, recv1, send2, recv2, state_sem, sq_send, sq_recv) = refs[21:31]
    (out_send1, out_send2, out_recv, pair_send, pair_recv) = refs[31:]
    kinds = len(g_refs)
    layers = g_refs[0].shape[0]
    rows = g_refs[0].shape[-2] // QUARTERS
    unit = kinds * rows

    me = lax.axis_index("dp")
    core = lax.rem(me, CORES)
    here = (lax.div(lax.div(me, CORES), side), lax.rem(lax.div(me, CORES), side))
    sibling = me + 1 - 2 * core

    def wrap(i):
        return lax.rem(i + 2 * side, side)

    def split(i):
        a, h = i // HALVES, i % HALVES
        return a, h, (1 - a) * here[0] + a * here[1], (1 - a) * here[1] + a * here[0]

    def chip(a, d, e):
        return (1 - a) * d + a * e, (1 - a) * e + a * d

    def device(a, d, e):
        x, y = chip(a, d, e)
        return (x * side + y) * CORES + core

    def remote(src, dst, send, recv, to):
        return pltpu.make_async_remote_copy(
            src_ref=src, dst_ref=dst, send_sem=send, recv_sem=recv, device_id={"dp": to}, device_id_type=pl.DeviceIdType.MESH
        )

    def quarter(i):
        return pl.ds(pl.multiple_of(i * rows, rows), rows)

    def away(s, h):
        return (2, 1 - 2 * h, 2 * h - 1, 0)[s]

    def load(a, h, d, w):
        lines = pl.ds((a * HALVES + h) * rows, rows)
        src = g_refs[w].at[:, d, :, core, lines, :] if a == 0 else g_refs[w].at[:, :, d, core, lines, :]
        return pltpu.make_async_copy(src, whole.at[0, a, h, d, :, :, pl.ds(w * rows, rows), :], load_sem.at[a, h, d, w])

    def swap(a, h, d, w):
        lines = pl.ds((a * HALVES + h) * rows, rows)
        src = g_refs[w].at[:, d, :, 1 - core, lines, :] if a == 0 else g_refs[w].at[:, :, d, 1 - core, lines, :]
        dst = whole.at[1, a, h, d, :, :, pl.ds(w * rows, rows), :]
        return remote(src, dst, swap_send.at[a, h, d, w], swap_recv.at[a, h, d, w], sibling)

    def first(a):
        return here[a]

    def dest(kind, a, h):
        return (wrap(first(a) + 2), wrap(first(a) + 1 - 2 * h), wrap(first(a) + 2 * h - 1), first(a))[kind]

    quarters = [(a, h) for a in range(AXES) for h in range(HALVES)]
    for kind in range(4):
        for a, h in quarters:
            for w in range(kinds):
                load(a, h, dest(kind, a, h), w).start()

    def state_copies():
        mine = (slice(None), here[0], here[1], core)
        for w in range(kinds):
            yield pltpu.make_async_copy(w_refs[w].at[mine], w_own.at[w], state_sem.at[0, w])
            yield pltpu.make_async_copy(m_refs[w], m_own.at[w], state_sem.at[1, w])
            yield pltpu.make_async_copy(v_refs[w], v_own.at[w], state_sem.at[2, w])

    barrier = pltpu.get_barrier_semaphore()

    def greet(i):
        pl.semaphore_signal(barrier, inc=1, device_id={"dp": lax.rem(me + 1 + i, n)}, device_id_type=pl.DeviceIdType.MESH)

    steps(n - 1, greet)
    pl.semaphore_wait(barrier, n - 1)

    for kind in range(4):
        for a, h in quarters:
            for w in range(kinds):
                swap(a, h, dest(kind, a, h), w).start()
    for copy in state_copies():
        copy.start()

    def wait_terms(kind, i):
        a, h, p, _ = split(i)
        d = wrap(p + away(kind, h))

        def one(w):
            pltpu.make_async_copy(whole.at[0, a, h, d, :, :, quarter(w), :], whole.at[0, a, h, d, :, :, quarter(w), :], load_sem.at[a, h, d, w]).wait()
            remote(
                whole.at[1, a, h, d, :, :, quarter(w), :],
                whole.at[1, a, h, d, :, :, quarter(w), :],
                swap_send.at[a, h, d, w],
                swap_recv.at[a, h, d, w],
                sibling,
            ).wait_recv()

        steps(kinds, one)

    def add(dst, *srcs):
        def piece(j):
            at = (j // kinds, quarter(j % kinds))
            total = srcs[0][at].astype(F32)
            for src in srcs[1:]:
                total += src[at].astype(F32)
            dst[at] = total.astype(BF16)

        steps(layers * kinds, piece)

    def toward(kind, p, h):
        return wrap(p + (2 * h - 1, 1 - 2 * h, 2 * h - 1)[kind])

    def pass1(kind, i, s):
        a, h, p, q = split(i)
        d, e = wrap(p + away(kind, h)), wrap(q + away(s, h))
        terms = whole.at[0, a, h, d, :, e]
        return terms, whole.at[1, a, h, d, :, e], remote(
            terms, land1.at[kind, a, h, s], send1.at[kind, a, h, s], recv1.at[kind, a, h, s], device(a, toward(kind, p, h), q)
        )

    for kind in range(3):

        def start1(i):
            a, h, _, _ = split(i)
            if kind < 2:
                wait_terms(kind, i)
            for s in range(4):
                terms, others, copy = pass1(kind, i, s)
                if kind == 2:
                    if s == 0:
                        wait_terms(kind, i)
                    pass1(0, i, s)[2].wait_recv()
                    add(terms, terms, others, land1.at[0, a, h, s])
                else:
                    add(terms, terms, others)
                copy.start()

        steps(QUARTERS, start1)

    def pass2(kind, i):
        a, h, p, q = split(i)
        e = wrap(q + away(kind, h))
        return remote(whole.at[0, a, h, p, :, e], land2.at[kind, a, h], send2.at[kind, a, h], recv2.at[kind, a, h], device(a, p, toward(kind, q, h)))

    for kind in range(3):

        def start2(i):
            a, h, p, q = split(i)
            if kind == 0:
                wait_terms(3, i)
            e = wrap(q + away(kind, h))
            pass1(1, i, kind)[2].wait_recv()
            pass1(2, i, kind)[2].wait_recv()
            terms = whole.at[0, a, h, p, :, e]
            srcs = [terms, whole.at[1, a, h, p, :, e], land1.at[1, a, h, kind], land1.at[2, a, h, kind]]
            if kind == 2:
                pass2(0, i).wait_recv()
                srcs.append(land2.at[0, a, h])
            add(terms, *srcs)
            pass2(kind, i).start()

        steps(QUARTERS, start2)

    def finish(i, total):
        a, h, p, q = split(i)
        pass1(1, i, 3)[2].wait_recv()
        pass1(2, i, 3)[2].wait_recv()
        pass2(1, i).wait_recv()
        pass2(2, i).wait_recv()
        srcs = [whole.at[k, a, h, p, :, q] for k in range(2)] + [land1.at[k, a, h, 3] for k in (1, 2)] + [land2.at[k, a, h] for k in (1, 2)]

        def piece(j, total):
            at = (j // kinds, quarter(j % kinds))
            g = srcs[0][at].astype(F32)
            for src in srcs[1:]:
                g += src[at].astype(F32)
            g = g.astype(BF16)
            grads[a, h, j // kinds, quarter(j % kinds)] = g
            g = g.astype(F32)
            return total + jnp.sum((g * g).reshape(rows // TILE, TILE, LANES), axis=0)

        return lax.fori_loop(0, layers * kinds, piece, total)

    squares[me] = lax.fori_loop(0, QUARTERS, finish, jnp.zeros((TILE, LANES), F32))

    def sent1(j):
        i, s = j // 4, j % 4
        a, h = i // HALVES, i % HALVES
        for kind in range(3):
            remote(land1.at[kind, a, h, s], land1.at[kind, a, h, s], send1.at[kind, a, h, s], recv1.at[kind, a, h, s], sibling).wait_send()

    steps(QUARTERS * 4, sent1)

    def sent2(i):
        for kind in range(3):
            pass2(kind, i).wait_send()

    steps(QUARTERS, sent2)

    def square(i):
        to, by = lax.rem(me + 1 + i, n), lax.rem(me + n - 1 - i, n)
        return (
            remote(squares.at[me], squares.at[me], sq_send.at[i], sq_recv.at[me], to),
            remote(squares.at[me], squares.at[by], sq_send.at[i], sq_recv.at[by], to),
        )

    steps(n - 1, lambda i: square(i)[0].start())
    for copy in state_copies():
        copy.wait()
    steps(n - 1, lambda i: square(i)[1].wait_recv())
    total = lax.fori_loop(0, n, lambda i, t: t + squares[i], jnp.zeros((TILE, LANES), F32))
    total = jnp.sum(jnp.sum(total, axis=0, keepdims=True), axis=1, keepdims=True)
    count = n * layers * kinds * QUARTERS * rows * LANES
    factor = jnp.minimum(1.0, 0.5 * lax.rsqrt(total / count + 1e-30))

    def out2(i, d, e, k, slot, r):
        a, h, p, q = split(i)
        return remote(whole.at[0, a, h, d, :, e], whole.at[0, a, h, d, :, e], out_send2.at[a, h, r, slot], out_recv.at[a, h, d, e], device(a, wrap(p + k), q))

    def out1(i, e, k, slot):
        a, h, p, q = split(i)
        return remote(whole.at[0, a, h, p, :, e], whole.at[0, a, h, p, :, e], out_send1.at[a, h, slot], out_recv.at[a, h, p, e], device(a, p, wrap(q + k)))

    def pair(i, d, e):
        a, h, _, _ = split(i)
        return remote(whole.at[0, a, h, d, :, e], whole.at[1, a, h, d, :, e], pair_send.at[a, h, d, e], pair_recv.at[a, h, d, e], sibling)

    def arrived(i, d, e):
        a, h, p, q = split(i)
        remote(whole.at[0, a, h, d, :, e], whole.at[0, a, h, d, :, e], out_send1.at[a, h, 0], out_recv.at[a, h, d, e], sibling).wait_recv()

    def update(i):
        a, h, p, q = split(i)

        def piece(j):
            layer, w = j // kinds, j % kinds
            at = (w, layer, pl.ds(pl.multiple_of(i * rows, rows), rows))
            g = grads[a, h, layer, quarter(w)].astype(F32) * factor
            w_old = w_own[at].astype(F32)
            m = 0.9 * m_own[at] + 0.1 * g
            v = 0.95 * v_own[at] + 0.05 * g * g
            step = m * lax.rsqrt(v + 1e-8) + 0.1 * w_old
            moments[(0, *at)] = m
            moments[(1, *at)] = v
            whole[0, a, h, p, layer, q, quarter(w)] = (w_old - 0.02 * step).astype(BF16)

        steps(layers * kinds, piece)
        out1(i, q, 2 * h - 1, 0).start()
        out2(i, p, q, 2 * h - 1, 0, 0).start()

    steps(QUARTERS, update)

    def own(i):
        _, h, p, q = split(i)
        out1(i, q, 1 - 2 * h, 1).start()
        out2(i, p, q, 1 - 2 * h, 1, 0).start()
        pair(i, p, q).start()

    steps(QUARTERS, own)

    def place(r, h):
        return (0, 1 - 2 * h, 2 * h - 1, 2)[r]

    def column(r):
        def run(i):
            _, h, p, q = split(i)
            e = wrap(q + place(r, h))
            arrived(i, p, e)
            if r == 1:
                out1(i, e, 2 * h - 1, 2).start()
            out2(i, p, e, 2 * h - 1, 0, r).start()
            out2(i, p, e, 1 - 2 * h, 1, r).start()
            pair(i, p, e).start()

        steps(QUARTERS, run)

    def beside(r):
        def run(i):
            _, h, p, q = split(i)
            e = wrap(q + place(r, h))
            d = wrap(p + 1 - 2 * h)
            arrived(i, d, e)
            out2(i, d, e, 2 * h - 1, 2, r).start()
            pair(i, d, e).start()
            d = wrap(p + 2 * h - 1)
            arrived(i, d, e)
            pair(i, d, e).start()

        steps(QUARTERS, run)

    def across(r):
        def run(i):
            _, h, p, q = split(i)
            d, e = wrap(p + 2), wrap(q + place(r, h))
            arrived(i, d, e)
            pair(i, d, e).start()

        steps(QUARTERS, run)

    column(1)
    column(2)
    beside(0)
    column(3)
    beside(1)
    beside(2)
    across(0)
    beside(3)
    across(1)
    across(2)
    across(3)

    def done(i):
        a, h, p, q = split(i)
        for slot in range(3):
            out1(i, q, 1, slot).wait_send()
            for r in range(4):
                out2(i, p, q, 1, slot, r).wait_send()

        def places(j):
            d, e = j // side, j % side
            pair(i, d, e).wait()

        steps(side * side, places)
        for d in range(side):
            for w in range(kinds):
                remote(
                    whole.at[1, a, h, d, :, :, quarter(w), :],
                    whole.at[1, a, h, d, :, :, quarter(w), :],
                    swap_send.at[a, h, d, w],
                    swap_recv.at[a, h, d, w],
                    sibling,
                ).wait_send()

    steps(QUARTERS, done)
    steps(n - 1, lambda i: square(i)[0].wait_send())


def write_kernel(side, whole, moments, *refs):
    w_refs, m_refs, v_refs, sem = refs[:3], refs[3:6], refs[6:9], refs[9]
    kinds = len(w_refs)
    rows = w_refs[0].shape[-2] // QUARTERS
    core = lax.rem(lax.axis_index("dp"), CORES)

    def copies(d, start):
        count = 0
        for k in range(CORES):
            c = core if k == 0 else 1 - core
            for a in range(AXES):
                for h in range(HALVES):
                    lines = pl.ds((a * HALVES + h) * rows, rows)
                    for w in range(kinds):
                        dst = w_refs[w].at[:, d, :, c, lines, :] if a == 0 else w_refs[w].at[:, :, d, c, lines, :]
                        copy = pltpu.make_async_copy(whole.at[k, a, h, d, :, :, pl.ds(w * rows, rows), :], dst, sem.at[d, count])
                        count += 1
                        copy.start() if start else copy.wait()

    def states():
        for w in range(kinds):
            yield pltpu.make_async_copy(moments.at[0, w], m_refs[w], sem.at[side, w])
            yield pltpu.make_async_copy(moments.at[1, w], v_refs[w], sem.at[side, kinds + w])

    for copy in states():
        copy.start()
    steps(side, lambda d: copies(d, True))
    for copy in states():
        copy.wait()
    steps(side, lambda d: copies(d, False))


def solution(mesh):
    n = mesh.shape["dp"]
    side = math.isqrt(n // CORES)

    def step(*arrays):
        terms, weights, m, v = (arrays[i : i + 3] for i in (0, 3, 6, 9))
        kinds, layers = len(weights), weights[0].shape[0]
        g = [tiled(t[0], side, side, CORES) for t in terms]
        w = [tiled(a, side, side, CORES) for a in weights]
        states = [tiled(a) for a in (*m, *v)]
        block = g[0].shape[-2]
        rows = block // QUARTERS
        unit = kinds * rows
        hbm, vmem = pl.BlockSpec(memory_space=pltpu.HBM), pl.BlockSpec(memory_space=pltpu.VMEM)
        dma = pltpu.SemaphoreType.DMA
        piece = (AXES, HALVES)
        whole, moments = pl.pallas_call(
            functools.partial(exchange_kernel, n, side),
            out_shape=(
                pltpu.VMEM((CORES, *piece, side, layers, side, unit, LANES), BF16),
                pltpu.VMEM((2, kinds, layers, block, LANES), F32),
            ),
            in_specs=[hbm] * 12,
            out_specs=(vmem, vmem),
            scratch_shapes=[
                pltpu.VMEM((3, *piece, side, layers, unit, LANES), BF16),
                pltpu.VMEM((3, *piece, layers, unit, LANES), BF16),
                pltpu.VMEM((*piece, layers, unit, LANES), BF16),
                pltpu.VMEM((kinds, layers, block, LANES), BF16),
                pltpu.VMEM((kinds, layers, block, LANES), F32),
                pltpu.VMEM((kinds, layers, block, LANES), F32),
                pltpu.VMEM((n, TILE, LANES), F32),
                dma((*piece, side, kinds)),
                dma((*piece, side, kinds)),
                dma((*piece, side, kinds)),
                dma((3, *piece, side)),
                dma((3, *piece, side)),
                dma((3, *piece)),
                dma((3, *piece)),
                dma((3, kinds)),
                dma((n,)),
                dma((n,)),
                dma((*piece, 3)),
                dma((*piece, side, 3)),
                dma((*piece, side, side)),
                dma((*piece, side, side)),
                dma((*piece, side, side)),
            ],
            compiler_params=pltpu.CompilerParams(collective_id=0, has_side_effects=True, vmem_limit_bytes=28 << 20),
            name="exchange",
        )(*g, *w, *states)
        out = pl.pallas_call(
            functools.partial(write_kernel, side),
            out_shape=tuple(jax.ShapeDtypeStruct(a.shape, a.dtype) for a in (*w, *states)),
            in_specs=[vmem] * 2,
            out_specs=(hbm,) * 9,
            scratch_shapes=[dma((side + 1, CORES * QUARTERS * kinds))],
            compiler_params=pltpu.CompilerParams(vmem_limit_bytes=1 << 20),
            name="write",
        )(*(pltpu.with_memory_space_constraint(a, pltpu.VMEM) for a in (whole, moments)))
        return tuple(untiled(o, a.shape) for o, a in zip(out, (*weights, *m, *v), strict=True))

    all_of, cut = P(None, None, None), P(None, "dp", None)
    return jax.shard_map(
        step,
        mesh=mesh,
        in_specs=(P(("rep", "dp"), None, None, None),) * 3 + (all_of,) * 3 + (cut,) * 6,
        out_specs=(P("rep", None, None),) * 3 + (P("rep", "dp", None),) * 6,
        check_vma=False,
    )
```

```python
import functools
import math

import jax
import jax.numpy as jnp
from jax import lax
from jax.experimental import pallas as pl
from jax.experimental.pallas import tpu as pltpu
from jax.sharding import PartitionSpec as P

LANES = 128
TILE = 8
CORES = 2
AXES = 2
HALVES = 2
QUARTERS = AXES * HALVES
F32, BF16 = jnp.float32, jnp.bfloat16


def tiled(a, *blocks):
    layers, rows, columns = a.shape
    a = a.reshape(layers, rows // TILE, TILE, columns // LANES, LANES).transpose(0, 1, 3, 2, 4)
    return a.reshape(layers, *blocks, rows * columns // (LANES * math.prod(blocks)), LANES)


def untiled(a, shape):
    layers, rows, columns = shape
    a = a.reshape(layers, rows // TILE, columns // LANES, TILE, LANES).transpose(0, 1, 3, 2, 4)
    return a.reshape(shape)


def steps(count, body):
    def run(i, carry):
        body(i)
        return carry

    lax.fori_loop(0, count, run, 0)


def exchange_kernel(n, side, *refs):
    g_refs, w_refs, m_refs, v_refs = (refs[i : i + 3] for i in (0, 3, 6, 9))
    whole, moments = refs[12:14]
    (land1, land2, grads, w_own, m_own, v_own, squares) = refs[14:21]
    load_sem, swap_first, swap_rest, arrivals, state_sem, sent = refs[21:]
    swap_sent, sent1, sent2, square_sent, square_came, out_sent1, out_sent2, pair_sent, pair_came = (sent.at[i] for i in range(9))
    kinds = len(g_refs)
    layers = g_refs[0].shape[0]
    rows = g_refs[0].shape[-2] // QUARTERS
    unit = kinds * rows

    me = lax.axis_index("dp")
    core = lax.rem(me, CORES)
    here = (lax.div(lax.div(me, CORES), side), lax.rem(lax.div(me, CORES), side))
    sibling = me + 1 - 2 * core

    def wrap(i):
        return lax.rem(i + 2 * side, side)

    def split(i):
        a, h = i // HALVES, i % HALVES
        return a, h, (1 - a) * here[0] + a * here[1], (1 - a) * here[1] + a * here[0]

    def chip(a, d, e):
        return (1 - a) * d + a * e, (1 - a) * e + a * d

    def device(a, d, e):
        x, y = chip(a, d, e)
        return (x * side + y) * CORES + core

    def remote(src, dst, send, recv, to):
        return pltpu.make_async_remote_copy(
            src_ref=src, dst_ref=dst, send_sem=send, recv_sem=recv, device_id={"dp": to}, device_id_type=pl.DeviceIdType.MESH
        )

    def quarter(i):
        return pl.ds(pl.multiple_of(i * rows, rows), rows)

    def away(s, h):
        return (2, 1 - 2 * h, 2 * h - 1, 0)[s]

    def wait(ref, sem):
        pltpu.make_async_copy(ref, ref, sem).wait()

    barrier = pltpu.get_barrier_semaphore()
    x, y = here
    beside_me = [sibling] + [device(0, wrap(x + i), wrap(y + j)) for i, j in ((1, 0), (-1, 0), (0, 1), (0, -1))]
    for to in beside_me:
        pl.semaphore_signal(barrier, inc=1, device_id={"dp": to}, device_id_type=pl.DeviceIdType.MESH)

    quarters = [(a, h) for a in range(AXES) for h in range(HALVES)]

    def blocks(of, kind, a, h, w):
        lines = pl.ds((a * HALVES + h) * rows, rows)
        d = wrap(here[a] + away(kind, h))
        src = g_refs[w].at[:, d, :, of, lines, :] if a == 0 else g_refs[w].at[:, :, d, of, lines, :]
        return src, (a, h, d, slice(None), slice(None), pl.ds(w * rows, rows), slice(None))

    for kind in range(4):
        for a, h in quarters:
            for w in range(kinds):
                src, at = blocks(core, kind, a, h, w)
                pltpu.make_async_copy(src, whole.at[(0, *at)], load_sem.at[kind]).start()

    def state_copies():
        mine = (slice(None), here[0], here[1], core)
        for w in range(kinds):
            yield pltpu.make_async_copy(w_refs[w].at[mine], w_own.at[w], state_sem.at[0])
            yield pltpu.make_async_copy(m_refs[w], m_own.at[w], state_sem.at[1])
            yield pltpu.make_async_copy(v_refs[w], v_own.at[w], state_sem.at[2])

    pl.semaphore_wait(barrier, len(beside_me))

    for s in range(4):

        def swap_one(i):
            a, h, p, q = split(i)
            d, e = wrap(p + 2), wrap(q + away(s, h))
            for w in range(kinds):
                src = g_refs[w].at[(slice(None), *chip(a, d, e), 1 - core, quarter(i), slice(None))]
                dst = whole.at[1, a, h, d, :, e, pl.ds(w * rows, rows), :]
                remote(src, dst, swap_sent, swap_first.at[i, s], sibling).start()

        steps(QUARTERS, swap_one)

    def swap_others():
        for kind in range(1, 4):
            for a, h in quarters:
                for w in range(kinds):
                    src, at = blocks(1 - core, kind, a, h, w)
                    remote(src, whole.at[(1, *at)], swap_sent, swap_rest.at[kind - 1], sibling).start()

    def wait_load(kind):
        wait(whole.at[0, :, :, 0], load_sem.at[kind])

    def wait_swap(kind):
        wait(whole.at[1, :, :, 0], swap_rest.at[kind - 1])

    def add(dst, *srcs):
        def piece(j):
            at = (j // kinds, quarter(j % kinds))
            total = srcs[0][at].astype(F32)
            for src in srcs[1:]:
                total += src[at].astype(F32)
            dst[at] = total.astype(BF16)

        steps(layers * kinds, piece)

    def toward(kind, p, h):
        return wrap(p + (2 * h - 1, 1 - 2 * h, 2 * h - 1)[kind])

    def arrival1(kind, a, h, s):
        return arrivals.at[a, h, (s, 8, 4 + s)[kind]]

    def pass1(kind, i, s):
        a, h, p, q = split(i)
        d, e = wrap(p + away(kind, h)), wrap(q + away(s, h))
        terms, others = whole.at[0, a, h, d, :, e], whole.at[1, a, h, d, :, e]
        to = device(a, toward(kind, p, h), q)
        return terms, others, remote(terms, land1.at[kind, a, h, s], sent1, arrival1(kind, a, h, s), to)

    wait_load(0)
    for s in range(4):

        def across_first(i):
            a, h, _, _ = split(i)
            wait(land2.at[0, 0, 0], swap_first.at[i, s])
            terms, others, copy = pass1(0, i, s)
            add(terms, terms, others)
            copy.start()

        steps(QUARTERS, across_first)
        if s == 0:
            swap_others()

    for kind in (1, 2):
        wait_load(kind)
        wait_swap(kind)
        for s in range(4):

            def start1(i):
                a, h, _, _ = split(i)
                terms, others, copy = pass1(kind, i, s)
                if kind == 2:
                    wait(land1.at[0, a, h, s], arrival1(0, a, h, s))
                    add(terms, terms, others, land1.at[0, a, h, s])
                else:
                    add(terms, terms, others)
                copy.start()

            steps(QUARTERS, start1)

    for copy in state_copies():
        copy.start()

    def arrival2(kind, a, h):
        return arrivals.at[a, h, 9 + kind]

    def pass2(kind, i):
        a, h, p, q = split(i)
        e = wrap(q + away(kind, h))
        return remote(whole.at[0, a, h, p, :, e], land2.at[kind, a, h], sent2, arrival2(kind, a, h), device(a, p, toward(kind, q, h)))

    wait_load(3)
    wait_swap(3)
    for kind in range(3):

        def start2(i):
            a, h, p, q = split(i)
            e = wrap(q + away(kind, h))
            if kind == 0:
                wait(land1.at[1, a, h], arrival1(1, a, h, 0))
            wait(land1.at[2, a, h, kind], arrival1(2, a, h, kind))
            terms = whole.at[0, a, h, p, :, e]
            srcs = [terms, whole.at[1, a, h, p, :, e], land1.at[1, a, h, kind], land1.at[2, a, h, kind]]
            if kind == 2:
                wait(land2.at[0, a, h], arrival2(0, a, h))
                srcs.append(land2.at[0, a, h])
            add(terms, *srcs)
            pass2(kind, i).start()

        steps(QUARTERS, start2)

    def finish(i, total):
        a, h, p, q = split(i)
        wait(land1.at[2, a, h, 3], arrival1(2, a, h, 3))
        for kind in (1, 2):
            wait(land2.at[kind, a, h], arrival2(kind, a, h))
        srcs = [whole.at[k, a, h, p, :, q] for k in range(2)] + [land1.at[k, a, h, 3] for k in (1, 2)] + [land2.at[k, a, h] for k in (1, 2)]

        def piece(j, total):
            at = (j // kinds, quarter(j % kinds))
            g = srcs[0][at].astype(F32)
            for src in srcs[1:]:
                g += src[at].astype(F32)
            g = g.astype(BF16)
            grads[a, h, j // kinds, quarter(j % kinds)] = g
            g = g.astype(F32)
            return total + jnp.sum((g * g).reshape(rows // TILE, TILE, LANES), axis=0)

        return lax.fori_loop(0, layers * kinds, piece, total)

    squares[me] = lax.fori_loop(0, QUARTERS, finish, jnp.zeros((TILE, LANES), F32))

    wait(land1, sent1)
    wait(land2, sent2)

    def square(i):
        remote(squares.at[me], squares.at[me], square_sent, square_came, lax.rem(me + 1 + i, n)).start()

    steps(n - 1, square)
    for i, ref in enumerate((w_own, m_own, v_own)):
        wait(ref, state_sem.at[i])
    wait(squares.at[pl.ds(0, n - 1)], square_came)
    total = lax.fori_loop(0, n, lambda i, t: t + squares[i], jnp.zeros((TILE, LANES), F32))
    total = jnp.sum(jnp.sum(total, axis=0, keepdims=True), axis=1, keepdims=True)
    count = n * layers * kinds * QUARTERS * rows * LANES
    factor = jnp.minimum(1.0, 0.5 * lax.rsqrt(total / count + 1e-30))

    def out2(i, d, e, k):
        a, h, p, q = split(i)
        ref = whole.at[0, a, h, d, :, e]
        remote(ref, ref, out_sent2, arrivals.at[a, h, d * side + e], device(a, wrap(p + k), q)).start()

    def out1(i, e, k):
        a, h, p, q = split(i)
        ref = whole.at[0, a, h, p, :, e]
        remote(ref, ref, out_sent1, arrivals.at[a, h, p * side + e], device(a, p, wrap(q + k))).start()

    def pair(i, d, e):
        a, h, _, _ = split(i)
        remote(whole.at[0, a, h, d, :, e], whole.at[1, a, h, d, :, e], pair_sent, pair_came, sibling).start()

    def arrived(i, d, e):
        a, h, _, _ = split(i)
        wait(whole.at[0, a, h, d, :, e], arrivals.at[a, h, d * side + e])

    def update(i):
        a, h, p, q = split(i)

        def piece(j):
            layer, w = j // kinds, j % kinds
            at = (w, layer, pl.ds(pl.multiple_of(i * rows, rows), rows))
            g = grads[a, h, layer, quarter(w)].astype(F32) * factor
            w_old = w_own[at].astype(F32)
            m = 0.9 * m_own[at] + 0.1 * g
            v = 0.95 * v_own[at] + 0.05 * g * g
            step = m * lax.rsqrt(v + 1e-8) + 0.1 * w_old
            moments[(0, *at)] = m
            moments[(1, *at)] = v
            whole[0, a, h, p, layer, q, quarter(w)] = (w_old - 0.02 * step).astype(BF16)

        steps(layers * kinds, piece)
        out1(i, q, 2 * h - 1)
        out2(i, p, q, 2 * h - 1)

    steps(QUARTERS, update)

    def own(i):
        _, h, p, q = split(i)
        out1(i, q, 1 - 2 * h)
        out2(i, p, q, 1 - 2 * h)
        pair(i, p, q)

    steps(QUARTERS, own)

    def place(r, h):
        return (0, 1 - 2 * h, 2 * h - 1, 2)[r]

    def column(r):
        def run(i):
            _, h, p, q = split(i)
            e = wrap(q + place(r, h))
            arrived(i, p, e)
            if r == 1:
                out1(i, e, 2 * h - 1)
            out2(i, p, e, 2 * h - 1)
            out2(i, p, e, 1 - 2 * h)
            pair(i, p, e)

        steps(QUARTERS, run)

    def beside(r):
        def run(i):
            _, h, p, q = split(i)
            e = wrap(q + place(r, h))
            d = wrap(p + 1 - 2 * h)
            arrived(i, d, e)
            out2(i, d, e, 2 * h - 1)
            pair(i, d, e)
            d = wrap(p + 2 * h - 1)
            arrived(i, d, e)
            pair(i, d, e)

        steps(QUARTERS, run)

    def across(r):
        def run(i):
            _, h, p, q = split(i)
            d, e = wrap(p + 2), wrap(q + place(r, h))
            arrived(i, d, e)
            pair(i, d, e)

        steps(QUARTERS, run)

    column(1)
    column(2)
    beside(0)
    column(3)
    beside(1)
    beside(2)
    across(0)
    beside(3)
    across(1)
    across(2)
    across(3)

    wait(whole.at[1], pair_came)
    wait(whole.at[0], pair_sent)
    wait(land1, out_sent2)
    wait(land2, out_sent1)
    wait(whole.at[1], swap_sent)
    wait(squares.at[pl.ds(0, n - 1)], square_sent)


def write_kernel(side, whole, moments, *refs):
    w_refs, m_refs, v_refs, sem = refs[:3], refs[3:6], refs[6:9], refs[9]
    kinds = len(w_refs)
    rows = w_refs[0].shape[-2] // QUARTERS
    core = lax.rem(lax.axis_index("dp"), CORES)

    def copies(d):
        for k in range(CORES):
            c = core if k == 0 else 1 - core
            for a in range(AXES):
                for h in range(HALVES):
                    lines = pl.ds((a * HALVES + h) * rows, rows)
                    for w in range(kinds):
                        dst = w_refs[w].at[:, d, :, c, lines, :] if a == 0 else w_refs[w].at[:, :, d, c, lines, :]
                        pltpu.make_async_copy(whole.at[k, a, h, d, :, :, pl.ds(w * rows, rows), :], dst, sem.at[0]).start()

    steps(side, copies)
    for w in range(kinds):
        pltpu.make_async_copy(moments.at[0, w], m_refs[w], sem.at[1]).start()
        pltpu.make_async_copy(moments.at[1, w], v_refs[w], sem.at[1]).start()
    pltpu.make_async_copy(whole, whole, sem.at[0]).wait()
    pltpu.make_async_copy(moments, moments, sem.at[1]).wait()


def solution(mesh):
    n = mesh.shape["dp"]
    side = math.isqrt(n // CORES)

    def step(*arrays):
        terms, weights, m, v = (arrays[i : i + 3] for i in (0, 3, 6, 9))
        kinds, layers = len(weights), weights[0].shape[0]
        g = [tiled(t[0], side, side, CORES) for t in terms]
        w = [tiled(a, side, side, CORES) for a in weights]
        states = [tiled(a) for a in (*m, *v)]
        block = g[0].shape[-2]
        rows = block // QUARTERS
        unit = kinds * rows
        hbm, vmem = pl.BlockSpec(memory_space=pltpu.HBM), pl.BlockSpec(memory_space=pltpu.VMEM)
        dma = pltpu.SemaphoreType.DMA
        piece = (AXES, HALVES)
        whole, moments = pl.pallas_call(
            functools.partial(exchange_kernel, n, side),
            out_shape=(
                pltpu.VMEM((CORES, *piece, side, layers, side, unit, LANES), BF16),
                pltpu.VMEM((2, kinds, layers, block, LANES), F32),
            ),
            in_specs=[hbm] * 12,
            out_specs=(vmem, vmem),
            scratch_shapes=[
                pltpu.VMEM((3, *piece, side, layers, unit, LANES), BF16),
                pltpu.VMEM((3, *piece, layers, unit, LANES), BF16),
                pltpu.VMEM((*piece, layers, unit, LANES), BF16),
                pltpu.VMEM((kinds, layers, block, LANES), BF16),
                pltpu.VMEM((kinds, layers, block, LANES), F32),
                pltpu.VMEM((kinds, layers, block, LANES), F32),
                pltpu.VMEM((n, TILE, LANES), F32),
                dma((4,)),
                dma((QUARTERS, 4)),
                dma((3,)),
                dma((*piece, side * side)),
                dma((3,)),
                dma((9,)),
            ],
            compiler_params=pltpu.CompilerParams(collective_id=0, has_side_effects=True, vmem_limit_bytes=33 << 20),
            name="exchange",
        )(*g, *w, *states)
        out = pl.pallas_call(
            functools.partial(write_kernel, side),
            out_shape=tuple(jax.ShapeDtypeStruct(a.shape, a.dtype) for a in (*w, *states)),
            in_specs=[vmem] * 2,
            out_specs=(hbm,) * 9,
            scratch_shapes=[dma((2,))],
            compiler_params=pltpu.CompilerParams(vmem_limit_bytes=1 << 20),
            name="write",
        )(*(pltpu.with_memory_space_constraint(a, pltpu.VMEM) for a in (whole, moments)))
        return tuple(untiled(o, a.shape) for o, a in zip(out, (*weights, *m, *v), strict=True))

    all_of, cut = P(None, None, None), P(None, "dp", None)
    return jax.shard_map(
        step,
        mesh=mesh,
        in_specs=(P(("rep", "dp"), None, None, None),) * 3 + (all_of,) * 3 + (cut,) * 6,
        out_specs=(P("rep", None, None),) * 3 + (P("rep", "dp", None),) * 6,
        check_vma=False,
    )
```

```python
import functools
import itertools
import math

import jax
import jax.numpy as jnp
from jax import lax
from jax.experimental import pallas as pl
from jax.experimental.pallas import tpu as pltpu
from jax.sharding import PartitionSpec as P

LANES = 128
TILE = 8
CORES = 2
AXES = 2
HALVES = 2
QUARTERS = AXES * HALVES
F32, BF16 = jnp.float32, jnp.bfloat16


def tiled(a, *blocks):
    layers, rows, columns = a.shape
    a = a.reshape(layers, rows // TILE, TILE, columns // LANES, LANES).transpose(0, 1, 3, 2, 4)
    return a.reshape(layers, *blocks, rows * columns // (LANES * math.prod(blocks)), LANES)


def untiled(a, shape):
    layers, rows, columns = shape
    a = a.reshape(layers, rows // TILE, columns // LANES, TILE, LANES).transpose(0, 1, 3, 2, 4)
    return a.reshape(shape)


def steps(count, body):
    def run(i, carry):
        body(i)
        return carry

    lax.fori_loop(0, count, run, 0)


def exchange_kernel(n, side, *refs):
    g_refs, w_refs, m_refs, v_refs = (refs[i : i + 3] for i in (0, 3, 6, 9))
    whole, moments = refs[12:14]
    land1, land2, partial, grads, w_own, m_own, v_own, squares = refs[14:22]
    load_sem, swap_first, swap_rest, arrivals, last, state_sem, sent = refs[22:]
    swap_sent, sent1, sent2, square_sent, square_came, out_sent1, out_sent2, pair_sent, pair_came = (sent.at[i] for i in range(9))
    kinds = len(g_refs)
    layers = g_refs[0].shape[0]
    rows = g_refs[0].shape[-2] // QUARTERS
    unit = kinds * rows

    me = lax.axis_index("dp")
    core = lax.rem(me, CORES)
    here = (lax.div(lax.div(me, CORES), side), lax.rem(lax.div(me, CORES), side))
    sibling = me + 1 - 2 * core

    def wrap(i):
        return lax.rem(i + 2 * side, side)

    def split(i):
        a, h = i // HALVES, i % HALVES
        return a, h, (1 - a) * here[0] + a * here[1], (1 - a) * here[1] + a * here[0]

    def chip(a, d, e):
        return (1 - a) * d + a * e, (1 - a) * e + a * d

    def device(a, d, e):
        x, y = chip(a, d, e)
        return (x * side + y) * CORES + core

    def remote(src, dst, send, recv, to):
        return pltpu.make_async_remote_copy(
            src_ref=src, dst_ref=dst, send_sem=send, recv_sem=recv, device_id={"dp": to}, device_id_type=pl.DeviceIdType.MESH
        )

    def quarter(i):
        return pl.ds(pl.multiple_of(i * rows, rows), rows)

    def away(s, h):
        return (2, 1 - 2 * h, 2 * h - 1, 0)[s]

    def wait(ref, sem):
        pltpu.make_async_copy(ref, ref, sem).wait()

    barrier = pltpu.get_barrier_semaphore()
    x, y = here
    beside_me = [sibling] + [device(0, wrap(x + i), wrap(y + j)) for i, j in ((1, 0), (-1, 0), (0, 1), (0, -1))]
    for to in beside_me:
        pl.semaphore_signal(barrier, inc=1, device_id={"dp": to}, device_id_type=pl.DeviceIdType.MESH)

    quarters = [(a, h) for a in range(AXES) for h in range(HALVES)]

    def blocks(of, kind, a, h, w):
        lines = pl.ds((a * HALVES + h) * rows, rows)
        d = wrap(here[a] + away(kind, h))
        src = g_refs[w].at[:, d, :, of, lines, :] if a == 0 else g_refs[w].at[:, :, d, of, lines, :]
        return src, (a, h, d, slice(None), slice(None), pl.ds(w * rows, rows), slice(None))

    def load(kind):
        for a, h in quarters:
            for w in range(kinds):
                src, at = blocks(core, kind, a, h, w)
                pltpu.make_async_copy(src, whole.at[(0, *at)], load_sem.at[kind]).start()

    def state_copies():
        mine = (slice(None), here[0], here[1], core)
        for w in range(kinds):
            yield pltpu.make_async_copy(w_refs[w].at[mine], w_own.at[w], state_sem.at[0])
            yield pltpu.make_async_copy(m_refs[w], m_own.at[w], state_sem.at[1])
            yield pltpu.make_async_copy(v_refs[w], v_own.at[w], state_sem.at[2])

    load(0)
    pl.semaphore_wait(barrier, len(beside_me))

    def swap_across(s):
        def one(i):
            a, h, p, q = split(i)
            d, e = wrap(p + 2), wrap(q + away(s, h))
            for w in range(kinds):
                src = g_refs[w].at[(slice(None), *chip(a, d, e), 1 - core, quarter(i), slice(None))]
                dst = whole.at[1, a, h, d, :, e, pl.ds(w * rows, rows), :]
                remote(src, dst, swap_sent, swap_first.at[i, s], sibling).start()

        steps(QUARTERS, one)

    def swap(kind):
        for a, h in quarters:
            for w in range(kinds):
                src, at = blocks(1 - core, kind, a, h, w)
                remote(src, whole.at[(1, *at)], swap_sent, swap_rest.at[kind - 1], sibling).start()

    swap_across(0)
    swap_across(1)

    def wait_load(kind):
        wait(whole.at[0, :, :, 0], load_sem.at[kind])

    def wait_swap(kind):
        wait(whole.at[1, :, :, 0], swap_rest.at[kind - 1])

    def add(dst, *srcs):
        def piece(j):
            at = (j // kinds, quarter(j % kinds))
            total = srcs[0][at].astype(F32)
            for src in srcs[1:]:
                total += src[at].astype(F32)
            dst[at] = total.astype(BF16)

        steps(layers * kinds, piece)

    def toward(kind, p, h):
        return wrap(p + (2 * h - 1, 1 - 2 * h, 2 * h - 1)[kind])

    def arrival1(kind, a, h, s):
        return arrivals.at[a, h, (s, 8, 4 + s)[kind]]

    def pass1(kind, i, s):
        a, h, p, q = split(i)
        d, e = wrap(p + away(kind, h)), wrap(q + away(s, h))
        terms, others = whole.at[0, a, h, d, :, e], whole.at[1, a, h, d, :, e]
        to = device(a, toward(kind, p, h), q)
        return terms, others, remote(terms, land1.at[kind, a, h, s], sent1, arrival1(kind, a, h, s), to)

    wait_load(0)
    for s in range(4):

        def across_first(i):
            a, h, _, _ = split(i)
            wait(land2.at[0, 0, 0], swap_first.at[i, s])
            terms, others, copy = pass1(0, i, s)
            add(terms, terms, others)
            copy.start()

        steps(QUARTERS, across_first)
        if s == 0:
            swap_across(2)
            swap_across(3)
            load(1)
        if s == 1:
            swap(1)
            load(2)
        if s == 2:
            swap(2)
            load(3)
            swap(3)

    for kind in (1, 2):
        wait_load(kind)
        wait_swap(kind)
        for s in range(4):

            def start1(i):
                a, h, _, _ = split(i)
                terms, others, copy = pass1(kind, i, s)
                if kind == 2:
                    wait(land1.at[0, a, h, s], arrival1(0, a, h, s))
                    add(terms, terms, others, land1.at[0, a, h, s])
                else:
                    add(terms, terms, others)
                copy.start()

            steps(QUARTERS, start1)

    for copy in state_copies():
        copy.start()

    def arrival2(kind, a, h):
        return arrivals.at[a, h, 9 + kind]

    def pass2(kind, i):
        a, h, p, q = split(i)
        e = wrap(q + away(kind, h))
        terms, to = whole.at[0, a, h, p, :, e], device(a, p, toward(kind, q, h))
        if kind < 2:
            return [remote(terms, land2.at[kind, a, h], sent2, arrival2(kind, a, h), to)]
        return [remote(terms.at[k], land2.at[kind, a, h, k], sent2, arrival2(kind + k, a, h), to) for k in range(layers)]

    wait_load(3)
    wait_swap(3)
    for kind in range(3):

        def start2(i):
            a, h, p, q = split(i)
            e = wrap(q + away(kind, h))
            if kind == 0:
                wait(land1.at[1, a, h], arrival1(1, a, h, 0))
            wait(land1.at[2, a, h, kind], arrival1(2, a, h, kind))
            terms = whole.at[0, a, h, p, :, e]
            srcs = [terms, whole.at[1, a, h, p, :, e], land1.at[1, a, h, kind], land1.at[2, a, h, kind]]
            if kind == 2:
                wait(land2.at[0, a, h], arrival2(0, a, h))
                srcs.append(land2.at[0, a, h])
            add(terms, *srcs)
            for copy in pass2(kind, i):
                copy.start()

        steps(QUARTERS, start2)

    def all_but_last(i):
        a, h, p, q = split(i)
        wait(land1.at[2, a, h, 3], arrival1(2, a, h, 3))
        wait(land2.at[1, a, h], arrival2(1, a, h))
        srcs = [whole.at[k, a, h, p, :, q] for k in range(2)] + [land1.at[k, a, h, 3] for k in (1, 2)] + [land2.at[1, a, h]]

        def piece(j):
            at = (j // kinds, quarter(j % kinds))
            partial[(a, h, *at)] = sum(src[at].astype(F32) for src in srcs)

        steps(layers * kinds, piece)

    steps(QUARTERS, all_but_last)

    def finish(i, total, layer):
        a, h, _, _ = split(i)
        wait(land2.at[2, a, h, layer], arrival2(2 + layer, a, h))

        def piece(j, total):
            at = (a, h, layer, quarter(j))
            g = (partial[at] + land2[(2, *at)].astype(F32)).astype(BF16)
            grads[at] = g
            g = g.astype(F32)
            return total + jnp.sum((g * g).reshape(rows // TILE, TILE, LANES), axis=0)

        return lax.fori_loop(0, kinds, piece, total)

    total = jnp.zeros((TILE, LANES), F32)
    for layer in range(layers):
        total = lax.fori_loop(0, QUARTERS, functools.partial(finish, layer=layer), total)
    squares[me] = jnp.sum(total, axis=0, keepdims=True)

    wait(land1, sent1)
    wait(land2, sent2)

    def far(place):
        return -min(place[0], side - place[0]) - min(place[1], side - place[1])

    for dx, dy, dc in sorted(itertools.product(range(side), range(side), range(CORES)), key=far):
        if not (dx or dy or dc):
            continue
        to = (wrap(x + dx) * side + wrap(y + dy)) * CORES + (core if dc == 0 else 1 - core)
        remote(squares.at[me], squares.at[me], square_sent, square_came, to).start()
    for i, ref in enumerate((w_own, m_own, v_own)):
        wait(ref, state_sem.at[i])
    wait(squares.at[pl.ds(0, n - 1)], square_came)
    total = lax.fori_loop(0, n, lambda i, t: t + squares[i], jnp.zeros((1, LANES), F32))
    total = jnp.sum(total, axis=1, keepdims=True)
    count = n * layers * kinds * QUARTERS * rows * LANES
    factor = jnp.minimum(1.0, 0.5 * lax.rsqrt(total / count + 1e-30))

    def out2(i, d, e, k):
        a, h, p, q = split(i)
        ref = whole.at[0, a, h, d, :, e]
        remote(ref, ref, out_sent2, arrivals.at[a, h, d * side + e], device(a, wrap(p + k), q)).start()

    def out1(i, e, k):
        a, h, p, q = split(i)
        ref = whole.at[0, a, h, p, :, e]
        remote(ref, ref, out_sent1, arrivals.at[a, h, p * side + e], device(a, p, wrap(q + k))).start()

    def pair(i, d, e):
        a, h, _, _ = split(i)
        remote(whole.at[0, a, h, d, :, e], whole.at[1, a, h, d, :, e], pair_sent, pair_came, sibling).start()

    def arrived(i, d, e):
        a, h, _, _ = split(i)
        wait(whole.at[0, a, h, d, :, e], arrivals.at[a, h, d * side + e])

    def stepped(i, j):
        a, h, _, _ = split(i)
        layer, w = j // kinds, j % kinds
        at = (w, layer, pl.ds(pl.multiple_of(i * rows, rows), rows))
        g = grads[a, h, layer, quarter(w)].astype(F32) * factor
        return at, 0.9 * m_own[at] + 0.1 * g, 0.95 * v_own[at] + 0.05 * g * g

    def update(i):
        a, h, p, q = split(i)

        def piece(j):
            at, m, v = stepped(i, j)
            w_old = w_own[at].astype(F32)
            step = m * lax.rsqrt(v + 1e-8) + 0.1 * w_old
            whole[0, a, h, p, j // kinds, q, quarter(j % kinds)] = (w_old - 0.02 * step).astype(BF16)

        steps(layers * kinds, piece)
        out1(i, q, 2 * h - 1)
        out2(i, p, q, 2 * h - 1)

    steps(QUARTERS, update)

    def own(i):
        _, h, p, q = split(i)
        out1(i, q, 1 - 2 * h)
        out2(i, p, q, 1 - 2 * h)
        pair(i, p, q)

    steps(QUARTERS, own)

    def keep(i):
        def piece(j):
            at, m, v = stepped(i, j)
            moments[(0, *at)] = m
            moments[(1, *at)] = v

        steps(layers * kinds, piece)

    steps(QUARTERS, keep)

    def place(r, h):
        return (0, 1 - 2 * h, 2 * h - 1, 2)[r]

    def column(r):
        def run(i):
            _, h, p, q = split(i)
            e = wrap(q + place(r, h))
            arrived(i, p, e)
            if r == 1:
                out1(i, e, 2 * h - 1)
            out2(i, p, e, 2 * h - 1)
            out2(i, p, e, 1 - 2 * h)
            pair(i, p, e)

        steps(QUARTERS, run)

    def beside(r):
        def run(i):
            a, h, p, q = split(i)
            e = wrap(q + place(r, h))
            d = wrap(p + 1 - 2 * h)
            arrived(i, d, e)
            if r < 3:
                out2(i, d, e, 2 * h - 1)
            else:
                for k in range(layers):
                    ref = whole.at[0, a, h, d, k, e]
                    remote(ref, ref, out_sent2, last.at[a, h, k], device(a, wrap(p + 2 * h - 1), q)).start()
            pair(i, d, e)
            d = wrap(p + 2 * h - 1)
            arrived(i, d, e)
            pair(i, d, e)

        steps(QUARTERS, run)

    def across(r):
        def run(i):
            _, h, p, q = split(i)
            d, e = wrap(p + 2), wrap(q + place(r, h))
            arrived(i, d, e)
            pair(i, d, e)

        steps(QUARTERS, run)

    def across_last(k):
        def run(i):
            a, h, p, q = split(i)
            d, e = wrap(p + 2), wrap(q + place(3, h))
            wait(whole.at[0, a, h, d, k, e], last.at[a, h, k])
            remote(whole.at[0, a, h, d, k, e], whole.at[1, a, h, d, k, e], pair_sent, pair_came, sibling).start()

        steps(QUARTERS, run)

    column(1)
    column(2)
    beside(0)
    column(3)
    beside(1)
    beside(2)
    across(0)
    beside(3)
    across(1)
    across(2)
    for k in range(layers):
        across_last(k)

    wait(whole.at[1], pair_came)
    wait(whole.at[0], pair_sent)
    wait(land1, out_sent2)
    wait(land2, out_sent1)
    wait(whole.at[1], swap_sent)
    wait(squares.at[pl.ds(0, n - 1)], square_sent)


def write_kernel(side, whole, moments, *refs):
    w_refs, m_refs, v_refs, sem = refs[:3], refs[3:6], refs[6:9], refs[9]
    kinds = len(w_refs)
    rows = w_refs[0].shape[-2] // QUARTERS
    core = lax.rem(lax.axis_index("dp"), CORES)

    def copies(d):
        for k in range(CORES):
            c = core if k == 0 else 1 - core
            for a in range(AXES):
                for h in range(HALVES):
                    lines = pl.ds((a * HALVES + h) * rows, rows)
                    for w in range(kinds):
                        dst = w_refs[w].at[:, d, :, c, lines, :] if a == 0 else w_refs[w].at[:, :, d, c, lines, :]
                        pltpu.make_async_copy(whole.at[k, a, h, d, :, :, pl.ds(w * rows, rows), :], dst, sem.at[0]).start()

    steps(side, copies)
    for w in range(kinds):
        pltpu.make_async_copy(moments.at[0, w], m_refs[w], sem.at[1]).start()
        pltpu.make_async_copy(moments.at[1, w], v_refs[w], sem.at[1]).start()
    pltpu.make_async_copy(whole, whole, sem.at[0]).wait()
    pltpu.make_async_copy(moments, moments, sem.at[1]).wait()


def solution(mesh):
    n = mesh.shape["dp"]
    side = math.isqrt(n // CORES)

    def step(*arrays):
        terms, weights, m, v = (arrays[i : i + 3] for i in (0, 3, 6, 9))
        kinds, layers = len(weights), weights[0].shape[0]
        g = [tiled(t[0], side, side, CORES) for t in terms]
        w = [tiled(a, side, side, CORES) for a in weights]
        states = [tiled(a) for a in (*m, *v)]
        block = g[0].shape[-2]
        rows = block // QUARTERS
        unit = kinds * rows
        hbm, vmem = pl.BlockSpec(memory_space=pltpu.HBM), pl.BlockSpec(memory_space=pltpu.VMEM)
        dma = pltpu.SemaphoreType.DMA
        piece = (AXES, HALVES)
        whole, moments = pl.pallas_call(
            functools.partial(exchange_kernel, n, side),
            out_shape=(
                pltpu.VMEM((CORES, *piece, side, layers, side, unit, LANES), BF16),
                pltpu.VMEM((2, kinds, layers, block, LANES), F32),
            ),
            in_specs=[hbm] * 12,
            out_specs=(vmem, vmem),
            scratch_shapes=[
                pltpu.VMEM((3, *piece, side, layers, unit, LANES), BF16),
                pltpu.VMEM((3, *piece, layers, unit, LANES), BF16),
                pltpu.VMEM((*piece, layers, unit, LANES), F32),
                pltpu.VMEM((*piece, layers, unit, LANES), BF16),
                pltpu.VMEM((kinds, layers, block, LANES), BF16),
                pltpu.VMEM((kinds, layers, block, LANES), F32),
                pltpu.VMEM((kinds, layers, block, LANES), F32),
                pltpu.VMEM((n, 1, LANES), F32),
                dma((4,)),
                dma((QUARTERS, 4)),
                dma((3,)),
                dma((*piece, side * side)),
                dma((*piece, layers)),
                dma((3,)),
                dma((9,)),
            ],
            compiler_params=pltpu.CompilerParams(collective_id=0, has_side_effects=True, vmem_limit_bytes=33 << 20),
            name="exchange",
        )(*g, *w, *states)
        out = pl.pallas_call(
            functools.partial(write_kernel, side),
            out_shape=tuple(jax.ShapeDtypeStruct(a.shape, a.dtype) for a in (*w, *states)),
            in_specs=[vmem] * 2,
            out_specs=(hbm,) * 9,
            scratch_shapes=[dma((2,))],
            compiler_params=pltpu.CompilerParams(vmem_limit_bytes=1 << 20),
            name="write",
        )(*(pltpu.with_memory_space_constraint(a, pltpu.VMEM) for a in (whole, moments)))
        return tuple(untiled(o, a.shape) for o, a in zip(out, (*weights, *m, *v), strict=True))

    all_of, cut = P(None, None, None), P(None, "dp", None)
    return jax.shard_map(
        step,
        mesh=mesh,
        in_specs=(P(("rep", "dp"), None, None, None),) * 3 + (all_of,) * 3 + (cut,) * 6,
        out_specs=(P("rep", None, None),) * 3 + (P("rep", "dp", None),) * 6,
        check_vma=False,
    )
```

```python
import functools
import itertools
import math

import jax
import jax.numpy as jnp
from jax import lax
from jax.experimental import pallas as pl
from jax.experimental.pallas import tpu as pltpu
from jax.sharding import PartitionSpec as P

LANES = 128
TILE = 8
CORES = 2
AXES = 2
HALVES = 2
QUARTERS = AXES * HALVES
F32, BF16 = jnp.float32, jnp.bfloat16


def tiled(a, *blocks):
    layers, rows, columns = a.shape
    a = a.reshape(layers, rows // TILE, TILE, columns // LANES, LANES).transpose(0, 1, 3, 2, 4)
    return a.reshape(layers, *blocks, rows * columns // (LANES * math.prod(blocks)), LANES)


def untiled(a, shape):
    layers, rows, columns = shape
    a = a.reshape(layers, rows // TILE, columns // LANES, TILE, LANES).transpose(0, 1, 3, 2, 4)
    return a.reshape(shape)


def steps(count, body):
    def run(i, carry):
        body(i)
        return carry

    lax.fori_loop(0, count, run, 0)


def exchange_kernel(n, side, *refs):
    g_refs, w_refs, m_refs, v_refs = (refs[i : i + 3] for i in (0, 3, 6, 9))
    whole, moments = refs[12:14]
    land1, land2, partial, grads, w_own, m_own, v_own, squares = refs[14:22]
    load_sem, swap_first, swap_next, swap_rest, arrivals, last, state_sem, sent = refs[22:]
    swap_sent, sent1, sent2, square_sent, square_came, out_sent1, out_sent2, pair_sent, pair_came = (sent.at[i] for i in range(9))
    kinds = len(g_refs)
    layers = g_refs[0].shape[0]
    rows = g_refs[0].shape[-2] // QUARTERS
    unit = kinds * rows

    me = lax.axis_index("dp")
    core = lax.rem(me, CORES)
    here = (lax.div(lax.div(me, CORES), side), lax.rem(lax.div(me, CORES), side))
    sibling = me + 1 - 2 * core

    def wrap(i):
        return lax.rem(i + 2 * side, side)

    def split(i):
        a, h = i // HALVES, i % HALVES
        return a, h, (1 - a) * here[0] + a * here[1], (1 - a) * here[1] + a * here[0]

    def chip(a, d, e):
        return (1 - a) * d + a * e, (1 - a) * e + a * d

    def device(a, d, e):
        x, y = chip(a, d, e)
        return (x * side + y) * CORES + core

    def remote(src, dst, send, recv, to):
        return pltpu.make_async_remote_copy(
            src_ref=src, dst_ref=dst, send_sem=send, recv_sem=recv, device_id={"dp": to}, device_id_type=pl.DeviceIdType.MESH
        )

    def quarter(i):
        return pl.ds(pl.multiple_of(i * rows, rows), rows)

    def away(s, h):
        return (2, 1 - 2 * h, 2 * h - 1, 0)[s]

    def wait(ref, sem):
        pltpu.make_async_copy(ref, ref, sem).wait()

    barrier = pltpu.get_barrier_semaphore()
    x, y = here
    beside_me = [sibling] + [device(0, wrap(x + i), wrap(y + j)) for i, j in ((1, 0), (-1, 0), (0, 1), (0, -1))]
    for to in beside_me:
        pl.semaphore_signal(barrier, inc=1, device_id={"dp": to}, device_id_type=pl.DeviceIdType.MESH)

    quarters = [(a, h) for a in range(AXES) for h in range(HALVES)]

    def blocks(of, kind, a, h, w):
        lines = pl.ds((a * HALVES + h) * rows, rows)
        d = wrap(here[a] + away(kind, h))
        src = g_refs[w].at[:, d, :, of, lines, :] if a == 0 else g_refs[w].at[:, :, d, of, lines, :]
        return src, (a, h, d, slice(None), slice(None), pl.ds(w * rows, rows), slice(None))

    def load(kind):
        for a, h in quarters:
            for w in range(kinds):
                src, at = blocks(core, kind, a, h, w)
                pltpu.make_async_copy(src, whole.at[(0, *at)], load_sem.at[kind]).start()

    def state_copies():
        mine = (slice(None), here[0], here[1], core)
        for w in range(kinds):
            yield pltpu.make_async_copy(w_refs[w].at[mine], w_own.at[w], state_sem.at[0])
            yield pltpu.make_async_copy(m_refs[w], m_own.at[w], state_sem.at[1])
            yield pltpu.make_async_copy(v_refs[w], v_own.at[w], state_sem.at[2])

    load(0)
    pl.semaphore_wait(barrier, len(beside_me))

    def swap_one(i, s, w, sem):
        a, h, p, q = split(i)
        d, e = wrap(p + 2), wrap(q + away(s, h))
        src = g_refs[w].at[(slice(None), *chip(a, d, e), 1 - core, quarter(i), slice(None))]
        remote(src, whole.at[1, a, h, d, :, e, pl.ds(w * rows, rows), :], swap_sent, sem, sibling).start()

    def swap_across(s):
        def one(i):
            for w in range(kinds):
                swap_one(i, s, w, swap_next.at[s - 1])

        steps(QUARTERS, one)

    def swap(kind):
        for a, h in quarters:
            for w in range(kinds):
                src, at = blocks(1 - core, kind, a, h, w)
                remote(src, whole.at[(1, *at)], swap_sent, swap_rest.at[kind - 1], sibling).start()

    for w in range(kinds):
        steps(QUARTERS, lambda i: swap_one(i, 0, w, swap_first.at[i, w]))
    swap_across(1)

    def wait_load(kind):
        wait(whole.at[0, :, :, 0], load_sem.at[kind])

    def wait_swap(kind):
        wait(whole.at[1, :, :, 0], swap_rest.at[kind - 1])

    def add(dst, *srcs):
        def piece(j):
            at = (j // kinds, quarter(j % kinds))
            total = srcs[0][at].astype(F32)
            for src in srcs[1:]:
                total += src[at].astype(F32)
            dst[at] = total.astype(BF16)

        steps(layers * kinds, piece)

    def toward(kind, p, h):
        return wrap(p + (2 * h - 1, 1 - 2 * h, 2 * h - 1)[kind])

    def arrival1(kind, a, h, s):
        return arrivals.at[a, h, (s, 8, 4 + s)[kind]]

    def pass1(kind, i, s):
        a, h, p, q = split(i)
        d, e = wrap(p + away(kind, h)), wrap(q + away(s, h))
        terms, others = whole.at[0, a, h, d, :, e], whole.at[1, a, h, d, :, e]
        to = device(a, toward(kind, p, h), q)
        return terms, others, remote(terms, land1.at[kind, a, h, s], sent1, arrival1(kind, a, h, s), to)

    def across_piece(i, w):
        a, h, p, q = split(i)
        d, e = wrap(p + 2), wrap(q + away(0, h))
        own, other = (whole.at[k, a, h, d, :, e, pl.ds(w * rows, rows)] for k in range(2))
        wait(land2.at[0, 0, 0, :, pl.ds(0, rows)], swap_first.at[i, w])

        def layer(j):
            own[j] = (own[j].astype(F32) + other[j].astype(F32)).astype(BF16)

        steps(layers, layer)
        to = device(a, toward(0, p, h), q)
        remote(own, land1.at[0, a, h, 0, :, pl.ds(w * rows, rows)], sent1, arrival1(0, a, h, 0), to).start()

    wait_load(0)
    for s in range(4):
        if s == 0:
            for w in range(kinds):
                steps(QUARTERS, lambda i: across_piece(i, w))
        else:
            wait(land2.at[0], swap_next.at[s - 1])

            def across_first(i):
                terms, others, copy = pass1(0, i, s)
                add(terms, terms, others)
                copy.start()

            steps(QUARTERS, across_first)
        if s == 0:
            swap_across(2)
            swap_across(3)
            load(1)
        if s == 1:
            swap(1)
            load(2)
        if s == 2:
            swap(2)
            load(3)
            swap(3)

    for kind in (1, 2):
        wait_load(kind)
        wait_swap(kind)
        for s in range(4):

            def start1(i):
                a, h, _, _ = split(i)
                terms, others, copy = pass1(kind, i, s)
                if kind == 2:
                    wait(land1.at[0, a, h, s], arrival1(0, a, h, s))
                    add(terms, terms, others, land1.at[0, a, h, s])
                else:
                    add(terms, terms, others)
                copy.start()

            steps(QUARTERS, start1)

    for copy in state_copies():
        copy.start()

    def arrival2(kind, a, h):
        return arrivals.at[a, h, 9 + kind]

    def pass2(kind, i):
        a, h, p, q = split(i)
        e = wrap(q + away(kind, h))
        terms, to = whole.at[0, a, h, p, :, e], device(a, p, toward(kind, q, h))
        if kind < 2:
            return [remote(terms, land2.at[kind, a, h], sent2, arrival2(kind, a, h), to)]
        pieces = [pl.ds(w * rows, rows) for w in range(kinds)]
        return [remote(terms.at[:, at], land2.at[kind, a, h, :, at], sent2, last.at[a, h, w], to) for w, at in enumerate(pieces)]

    wait_load(3)
    wait_swap(3)
    for kind in range(3):

        def start2(i):
            a, h, p, q = split(i)
            e = wrap(q + away(kind, h))
            if kind == 0:
                wait(land1.at[1, a, h], arrival1(1, a, h, 0))
            wait(land1.at[2, a, h, kind], arrival1(2, a, h, kind))
            terms = whole.at[0, a, h, p, :, e]
            srcs = [terms, whole.at[1, a, h, p, :, e], land1.at[1, a, h, kind], land1.at[2, a, h, kind]]
            if kind == 2:
                wait(land2.at[0, a, h], arrival2(0, a, h))
                srcs.append(land2.at[0, a, h])
            add(terms, *srcs)
            for copy in pass2(kind, i):
                copy.start()

        steps(QUARTERS, start2)

    def all_but_last(i):
        a, h, p, q = split(i)
        wait(land1.at[2, a, h, 3], arrival1(2, a, h, 3))
        wait(land2.at[1, a, h], arrival2(1, a, h))
        srcs = [whole.at[k, a, h, p, :, q] for k in range(2)] + [land1.at[k, a, h, 3] for k in (1, 2)] + [land2.at[1, a, h]]

        def piece(j):
            at = (j // kinds, quarter(j % kinds))
            partial[(a, h, *at)] = sum(src[at].astype(F32) for src in srcs)

        steps(layers * kinds, piece)

    steps(QUARTERS, all_but_last)

    def finish(i, total, w):
        a, h, _, _ = split(i)
        wait(land2.at[2, a, h, :, pl.ds(w * rows, rows)], last.at[a, h, w])

        def piece(j, total):
            at = (a, h, j, pl.ds(w * rows, rows))
            g = (partial[at] + land2[(2, *at)].astype(F32)).astype(BF16)
            grads[at] = g
            g = g.astype(F32)
            return total + jnp.sum((g * g).reshape(rows // TILE, TILE, LANES), axis=0)

        return lax.fori_loop(0, layers, piece, total)

    total = jnp.zeros((TILE, LANES), F32)
    for w in range(kinds):
        total = lax.fori_loop(0, QUARTERS, functools.partial(finish, w=w), total)
    squares[me] = jnp.sum(total, axis=0, keepdims=True)

    wait(land1, sent1)
    wait(land2, sent2)

    def far(place):
        return -min(place[0], side - place[0]) - min(place[1], side - place[1])

    for dx, dy, dc in sorted(itertools.product(range(side), range(side), range(CORES)), key=far):
        if not (dx or dy or dc):
            continue
        to = (wrap(x + dx) * side + wrap(y + dy)) * CORES + (core if dc == 0 else 1 - core)
        remote(squares.at[me], squares.at[me], square_sent, square_came, to).start()
    for i, ref in enumerate((w_own, m_own, v_own)):
        wait(ref, state_sem.at[i])
    wait(squares.at[pl.ds(0, n - 1)], square_came)
    total = lax.fori_loop(0, n, lambda i, t: t + squares[i], jnp.zeros((1, LANES), F32))
    total = jnp.sum(total, axis=1, keepdims=True)
    count = n * layers * kinds * QUARTERS * rows * LANES
    factor = jnp.minimum(1.0, 0.5 * lax.rsqrt(total / count + 1e-30))

    def out2(i, d, e, k, far=1):
        a, h, p, q = split(i)
        ref = whole.at[0, a, h, d, :, e]
        remote(ref, ref, out_sent2, arrivals.at[a, h, far * side + e], device(a, wrap(p + k), q)).start()

    def out1(i, e, k):
        a, h, p, q = split(i)
        ref = whole.at[0, a, h, p, :, e]
        remote(ref, ref, out_sent1, arrivals.at[a, h, e], device(a, p, wrap(q + k))).start()

    def pair(i, d, e):
        a, h, _, _ = split(i)
        remote(whole.at[0, a, h, d, :, e], whole.at[1, a, h, d, :, e], pair_sent, pair_came, sibling).start()

    def arrived(i, e, far):
        a, h, _, _ = split(i)
        wait(land2.at[0, 0] if far == 1 else land2.at[0, 0, 0], arrivals.at[a, h, far * side + e])

    def stepped(i, j):
        a, h, _, _ = split(i)
        layer, w = j // kinds, j % kinds
        at = (w, layer, pl.ds(pl.multiple_of(i * rows, rows), rows))
        g = grads[a, h, layer, quarter(w)].astype(F32) * factor
        return at, 0.9 * m_own[at] + 0.1 * g, 0.95 * v_own[at] + 0.05 * g * g

    def update(i, w):
        a, h, p, q = split(i)

        def layer(j):
            at, m, v = stepped(i, j * kinds + w)
            w_old = w_own[at].astype(F32)
            step = m * lax.rsqrt(v + 1e-8) + 0.1 * w_old
            whole[0, a, h, p, j, q, pl.ds(w * rows, rows)] = (w_old - 0.02 * step).astype(BF16)

        steps(layers, layer)
        ref = whole.at[0, a, h, p, :, q, pl.ds(w * rows, rows)]
        k = 2 * h - 1
        remote(ref, ref, out_sent1, arrivals.at[a, h, q], device(a, p, wrap(q + k))).start()
        remote(ref, ref, out_sent2, arrivals.at[a, h, side + q], device(a, wrap(p + k), q)).start()

    for w in range(kinds):
        steps(QUARTERS, lambda i: update(i, w))

    def own(i):
        _, h, p, q = split(i)
        out1(i, q, 1 - 2 * h)
        out2(i, p, q, 1 - 2 * h)
        pair(i, p, q)

    steps(QUARTERS, own)

    def keep(i):
        def piece(j):
            at, m, v = stepped(i, j)
            moments[(0, *at)] = m
            moments[(1, *at)] = v

        steps(layers * kinds, piece)

    steps(QUARTERS, keep)

    def place(r, h):
        return (0, 1 - 2 * h, 2 * h - 1, 2)[r]

    def column(r):
        def run(i):
            _, h, p, q = split(i)
            e = wrap(q + place(r, h))
            arrived(i, e, 0)
            if r == 1:
                out1(i, e, 2 * h - 1)
            out2(i, p, e, 2 * h - 1)
            out2(i, p, e, 1 - 2 * h)
            pair(i, p, e)

        steps(QUARTERS, run)

    def beside(r):
        def run(i):
            a, h, p, q = split(i)
            e = wrap(q + place(r, h))
            d = wrap(p + 1 - 2 * h)
            arrived(i, e, 1)
            if r < 3:
                out2(i, d, e, 2 * h - 1, 2)
            else:
                for w in range(kinds):
                    ref = whole.at[0, a, h, d, :, e, pl.ds(w * rows, rows)]
                    remote(ref, ref, out_sent2, last.at[a, h, w], device(a, wrap(p + 2 * h - 1), q)).start()
            pair(i, d, e)
            pair(i, wrap(p + 2 * h - 1), e)

        steps(QUARTERS, run)

    def across(r):
        def run(i):
            _, h, p, q = split(i)
            e = wrap(q + place(r, h))
            arrived(i, e, 2)
            pair(i, wrap(p + 2), e)

        steps(QUARTERS, run)

    def across_last(i, w):
        a, h, p, q = split(i)
        at = (a, h, wrap(p + 2), slice(None), wrap(q + place(3, h)), pl.ds(w * rows, rows))
        wait(land2.at[0, 0, 0, :, pl.ds(0, rows)], last.at[a, h, w])
        remote(whole.at[(0, *at)], whole.at[(1, *at)], pair_sent, pair_came, sibling).start()

    column(1)
    column(2)
    beside(0)
    column(3)
    beside(1)
    beside(2)
    across(0)
    beside(3)
    across(1)
    across(2)
    for w in range(kinds):
        steps(QUARTERS, lambda i: across_last(i, w))

    wait(whole.at[1], pair_came)
    wait(whole.at[0], pair_sent)
    wait(land1, out_sent2)
    wait(land2, out_sent1)
    wait(whole.at[1], swap_sent)
    wait(squares.at[pl.ds(0, n - 1)], square_sent)


def write_kernel(side, whole, moments, *refs):
    w_refs, m_refs, v_refs, sem = refs[:3], refs[3:6], refs[6:9], refs[9]
    kinds = len(w_refs)
    rows = w_refs[0].shape[-2] // QUARTERS
    core = lax.rem(lax.axis_index("dp"), CORES)

    def copies(d):
        for k in range(CORES):
            c = core if k == 0 else 1 - core
            for a in range(AXES):
                for h in range(HALVES):
                    lines = pl.ds((a * HALVES + h) * rows, rows)
                    for w in range(kinds):
                        dst = w_refs[w].at[:, d, :, c, lines, :] if a == 0 else w_refs[w].at[:, :, d, c, lines, :]
                        pltpu.make_async_copy(whole.at[k, a, h, d, :, :, pl.ds(w * rows, rows), :], dst, sem.at[0]).start()

    steps(side, copies)
    for w in range(kinds):
        pltpu.make_async_copy(moments.at[0, w], m_refs[w], sem.at[1]).start()
        pltpu.make_async_copy(moments.at[1, w], v_refs[w], sem.at[1]).start()
    pltpu.make_async_copy(whole, whole, sem.at[0]).wait()
    pltpu.make_async_copy(moments, moments, sem.at[1]).wait()


def solution(mesh):
    n = mesh.shape["dp"]
    side = math.isqrt(n // CORES)

    def step(*arrays):
        terms, weights, m, v = (arrays[i : i + 3] for i in (0, 3, 6, 9))
        kinds, layers = len(weights), weights[0].shape[0]
        g = [tiled(t[0], side, side, CORES) for t in terms]
        w = [tiled(a, side, side, CORES) for a in weights]
        states = [tiled(a) for a in (*m, *v)]
        block = g[0].shape[-2]
        rows = block // QUARTERS
        unit = kinds * rows
        hbm, vmem = pl.BlockSpec(memory_space=pltpu.HBM), pl.BlockSpec(memory_space=pltpu.VMEM)
        dma = pltpu.SemaphoreType.DMA
        piece = (AXES, HALVES)
        whole, moments = pl.pallas_call(
            functools.partial(exchange_kernel, n, side),
            out_shape=(
                pltpu.VMEM((CORES, *piece, side, layers, side, unit, LANES), BF16),
                pltpu.VMEM((2, kinds, layers, block, LANES), F32),
            ),
            in_specs=[hbm] * 12,
            out_specs=(vmem, vmem),
            scratch_shapes=[
                pltpu.VMEM((3, *piece, side, layers, unit, LANES), BF16),
                pltpu.VMEM((3, *piece, layers, unit, LANES), BF16),
                pltpu.VMEM((*piece, layers, unit, LANES), F32),
                pltpu.VMEM((*piece, layers, unit, LANES), BF16),
                pltpu.VMEM((kinds, layers, block, LANES), BF16),
                pltpu.VMEM((kinds, layers, block, LANES), F32),
                pltpu.VMEM((kinds, layers, block, LANES), F32),
                pltpu.VMEM((n, 1, LANES), F32),
                dma((4,)),
                dma((QUARTERS, kinds)),
                dma((3,)),
                dma((3,)),
                dma((*piece, 3 * side)),
                dma((*piece, kinds)),
                dma((3,)),
                dma((9,)),
            ],
            compiler_params=pltpu.CompilerParams(collective_id=0, has_side_effects=True, vmem_limit_bytes=33 << 20),
            name="exchange",
        )(*g, *w, *states)
        out = pl.pallas_call(
            functools.partial(write_kernel, side),
            out_shape=tuple(jax.ShapeDtypeStruct(a.shape, a.dtype) for a in (*w, *states)),
            in_specs=[vmem] * 2,
            out_specs=(hbm,) * 9,
            scratch_shapes=[dma((2,))],
            compiler_params=pltpu.CompilerParams(vmem_limit_bytes=1 << 20),
            name="write",
        )(*(pltpu.with_memory_space_constraint(a, pltpu.VMEM) for a in (whole, moments)))
        return tuple(untiled(o, a.shape) for o, a in zip(out, (*weights, *m, *v), strict=True))

    all_of, cut = P(None, None, None), P(None, "dp", None)
    return jax.shard_map(
        step,
        mesh=mesh,
        in_specs=(P(("rep", "dp"), None, None, None),) * 3 + (all_of,) * 3 + (cut,) * 6,
        out_specs=(P("rep", None, None),) * 3 + (P("rep", "dp", None),) * 6,
        check_vma=False,
    )
```

```python
import functools
import itertools
import math

import jax
import jax.numpy as jnp
from jax import lax
from jax.experimental import pallas as pl
from jax.experimental.pallas import tpu as pltpu
from jax.sharding import PartitionSpec as P

LANES = 128
TILE = 8
KINDS = 3
CORES = 2
AXES = 2
HALVES = 2
QUARTERS = AXES * HALVES
F32, BF16 = jnp.float32, jnp.bfloat16


def tiled(a, *blocks):
    layers, rows, columns = a.shape
    a = a.reshape(layers, rows // TILE, TILE, columns // LANES, LANES).transpose(0, 1, 3, 2, 4)
    return a.reshape(layers, *blocks, rows * columns // (LANES * math.prod(blocks)), LANES)


def untiled(a, shape):
    layers, rows, columns = shape
    a = a.reshape(layers, rows // TILE, columns // LANES, TILE, LANES).transpose(0, 1, 3, 2, 4)
    return a.reshape(shape)


def steps(count, body):
    def run(i, carry):
        body(i)
        return carry

    lax.fori_loop(0, count, run, 0)


def exchange_kernel(n, side, *refs):
    kinds, dma, piece = KINDS, pltpu.SemaphoreType.DMA, (AXES, HALVES)
    pl.run_scoped(
        lambda *sems: exchange(n, side, *refs, *sems),
        dma((4,)),
        dma((3,)),
        dma((QUARTERS, kinds)),
        dma((3,)),
        dma((3,)),
        dma((*piece, 3 * side)),
        dma((*piece, kinds)),
        dma((3,)),
        dma((9,)),
    )


def exchange(n, side, *refs):
    g_refs, w_refs, m_refs, v_refs = (refs[i : i + 3] for i in (0, 3, 6, 9))
    whole, moments = refs[12:14]
    land1, land2, partial, grads, w_own, m_own, v_own, squares = refs[14:22]
    load_first, load_sem, swap_first, swap_next, swap_rest, arrivals, last, state_sem, sent = refs[22:]
    swap_sent, sent1, sent2, square_sent, square_came, out_sent1, out_sent2, pair_sent, pair_came = (sent.at[i] for i in range(9))
    kinds = len(g_refs)
    layers = g_refs[0].shape[0]
    rows = g_refs[0].shape[-2] // QUARTERS
    unit = kinds * rows

    me = lax.axis_index("dp")
    core = lax.rem(me, CORES)
    here = (lax.div(lax.div(me, CORES), side), lax.rem(lax.div(me, CORES), side))
    sibling = me + 1 - 2 * core

    def wrap(i):
        return lax.rem(i + 2 * side, side)

    def split(i):
        a, h = i // HALVES, i % HALVES
        return a, h, (1 - a) * here[0] + a * here[1], (1 - a) * here[1] + a * here[0]

    def chip(a, d, e):
        return (1 - a) * d + a * e, (1 - a) * e + a * d

    def device(a, d, e):
        x, y = chip(a, d, e)
        return (x * side + y) * CORES + core

    def remote(src, dst, send, recv, to):
        return pltpu.make_async_remote_copy(
            src_ref=src, dst_ref=dst, send_sem=send, recv_sem=recv, device_id={"dp": to}, device_id_type=pl.DeviceIdType.MESH
        )

    def quarter(i):
        return pl.ds(pl.multiple_of(i * rows, rows), rows)

    def away(s, h):
        return (2, 1 - 2 * h, 2 * h - 1, 0)[s]

    def wait(ref, sem):
        pltpu.make_async_copy(ref, ref, sem).wait()

    barrier = pltpu.get_barrier_semaphore()
    x, y = here
    beside_me = [sibling] + [device(0, wrap(x + i), wrap(y + j)) for i, j in ((1, 0), (-1, 0), (0, 1), (0, -1))]
    for to in beside_me:
        pl.semaphore_signal(barrier, inc=1, device_id={"dp": to}, device_id_type=pl.DeviceIdType.MESH)

    quarters = [(a, h) for a in range(AXES) for h in range(HALVES)]

    def blocks(of, kind, a, h, w):
        lines = pl.ds((a * HALVES + h) * rows, rows)
        d = wrap(here[a] + away(kind, h))
        src = g_refs[w].at[:, d, :, of, lines, :] if a == 0 else g_refs[w].at[:, :, d, of, lines, :]
        return src, (a, h, d, slice(None), slice(None), pl.ds(w * rows, rows), slice(None))

    def load(kind):
        for a, h in quarters:
            for w in range(kinds):
                src, at = blocks(core, kind, a, h, w)
                pltpu.make_async_copy(src, whole.at[(0, *at)], load_sem.at[kind - 1]).start()

    def state_copies():
        mine = (slice(None), here[0], here[1], core)
        for w in range(kinds):
            yield pltpu.make_async_copy(w_refs[w].at[mine], w_own.at[w], state_sem.at[0])
            yield pltpu.make_async_copy(m_refs[w], m_own.at[w], state_sem.at[1])
            yield pltpu.make_async_copy(v_refs[w], v_own.at[w], state_sem.at[2])

    def across_at(i, s, w, of):
        a, h, p, q = split(i)
        d, e = wrap(p + 2), wrap(q + away(s, h))
        return g_refs[w].at[(slice(None), *chip(a, d, e), of, quarter(i), slice(None))], (a, h, d, slice(None), e, pl.ds(w * rows, rows))

    def load_across(s):
        def one(i):
            for w in range(kinds):
                src, at = across_at(i, s, w, core)
                pltpu.make_async_copy(src, whole.at[(0, *at)], load_first.at[s]).start()

        steps(QUARTERS, one)

    load_across(0)
    pl.semaphore_wait(barrier, len(beside_me))

    def swap_one(i, s, w, sem):
        src, at = across_at(i, s, w, 1 - core)
        remote(src, whole.at[(1, *at)], swap_sent, sem, sibling).start()

    def swap_across(s):
        def one(i):
            for w in range(kinds):
                swap_one(i, s, w, swap_next.at[s - 1])

        steps(QUARTERS, one)

    def swap(kind):
        for a, h in quarters:
            for w in range(kinds):
                src, at = blocks(1 - core, kind, a, h, w)
                remote(src, whole.at[(1, *at)], swap_sent, swap_rest.at[kind - 1], sibling).start()

    for w in range(kinds):
        steps(QUARTERS, lambda i: swap_one(i, 0, w, swap_first.at[i, w]))
    load_across(1)
    swap_across(1)

    def wait_load(kind):
        wait(whole.at[0, :, :, 0], load_sem.at[kind - 1])

    def wait_swap(kind):
        wait(whole.at[1, :, :, 0], swap_rest.at[kind - 1])

    def add(dst, *srcs):
        def piece(j):
            at = (j // kinds, quarter(j % kinds))
            total = srcs[0][at].astype(F32)
            for src in srcs[1:]:
                total += src[at].astype(F32)
            dst[at] = total.astype(BF16)

        steps(layers * kinds, piece)

    def toward(kind, p, h):
        return wrap(p + (2 * h - 1, 1 - 2 * h, 2 * h - 1)[kind])

    def arrival1(kind, a, h, s):
        return arrivals.at[a, h, (s, 8, 4 + s)[kind]]

    def pass1(kind, i, s):
        a, h, p, q = split(i)
        d, e = wrap(p + away(kind, h)), wrap(q + away(s, h))
        terms, others = whole.at[0, a, h, d, :, e], whole.at[1, a, h, d, :, e]
        to = device(a, toward(kind, p, h), q)
        return terms, others, remote(terms, land1.at[kind, a, h, s], sent1, arrival1(kind, a, h, s), to)

    def across_piece(i, w):
        a, h, p, q = split(i)
        d, e = wrap(p + 2), wrap(q + away(0, h))
        own, other = (whole.at[k, a, h, d, :, e, pl.ds(w * rows, rows)] for k in range(2))
        wait(land2.at[0, 0, 0, :, pl.ds(0, rows)], swap_first.at[i, w])

        def layer(j):
            own[j] = (own[j].astype(F32) + other[j].astype(F32)).astype(BF16)

        steps(layers, layer)
        to = device(a, toward(0, p, h), q)
        remote(own, land1.at[0, a, h, 0, :, pl.ds(w * rows, rows)], sent1, arrival1(0, a, h, 0), to).start()

    for s in range(4):
        wait(land2.at[0], load_first.at[s])
        if s == 0:
            for w in range(kinds):
                steps(QUARTERS, lambda i: across_piece(i, w))
        else:
            wait(land2.at[0], swap_next.at[s - 1])

            def across_first(i):
                terms, others, copy = pass1(0, i, s)
                add(terms, terms, others)
                copy.start()

            steps(QUARTERS, across_first)
        if s == 0:
            load_across(2)
            swap_across(2)
            load_across(3)
            swap_across(3)
            load(1)
        if s == 1:
            swap(1)
            load(2)
        if s == 2:
            swap(2)
            load(3)
            swap(3)

    for kind in (1, 2):
        wait_load(kind)
        wait_swap(kind)
        for s in range(4):

            def start1(i):
                a, h, _, _ = split(i)
                terms, others, copy = pass1(kind, i, s)
                if kind == 2:
                    wait(land1.at[0, a, h, s], arrival1(0, a, h, s))
                    add(terms, terms, others, land1.at[0, a, h, s])
                else:
                    add(terms, terms, others)
                copy.start()

            steps(QUARTERS, start1)

    for copy in state_copies():
        copy.start()

    def arrival2(kind, a, h):
        return arrivals.at[a, h, 9 + kind]

    def pass2(kind, i):
        a, h, p, q = split(i)
        e = wrap(q + away(kind, h))
        terms, to = whole.at[0, a, h, p, :, e], device(a, p, toward(kind, q, h))
        if kind < 2:
            return [remote(terms, land2.at[kind, a, h], sent2, arrival2(kind, a, h), to)]
        pieces = [pl.ds(w * rows, rows) for w in range(kinds)]
        return [remote(terms.at[:, at], land2.at[kind, a, h, :, at], sent2, last.at[a, h, w], to) for w, at in enumerate(pieces)]

    wait_load(3)
    wait_swap(3)
    for kind in range(3):

        def start2(i):
            a, h, p, q = split(i)
            e = wrap(q + away(kind, h))
            if kind == 0:
                wait(land1.at[1, a, h], arrival1(1, a, h, 0))
            wait(land1.at[2, a, h, kind], arrival1(2, a, h, kind))
            terms = whole.at[0, a, h, p, :, e]
            srcs = [terms, whole.at[1, a, h, p, :, e], land1.at[1, a, h, kind], land1.at[2, a, h, kind]]
            if kind == 2:
                wait(land2.at[0, a, h], arrival2(0, a, h))
                srcs.append(land2.at[0, a, h])
            add(terms, *srcs)
            for copy in pass2(kind, i):
                copy.start()

        steps(QUARTERS, start2)

    def all_but_last(i):
        a, h, p, q = split(i)
        wait(land1.at[2, a, h, 3], arrival1(2, a, h, 3))
        wait(land2.at[1, a, h], arrival2(1, a, h))
        srcs = [whole.at[k, a, h, p, :, q] for k in range(2)] + [land1.at[k, a, h, 3] for k in (1, 2)] + [land2.at[1, a, h]]

        def piece(j):
            at = (j // kinds, quarter(j % kinds))
            partial[(a, h, *at)] = sum(src[at].astype(F32) for src in srcs)

        steps(layers * kinds, piece)

    steps(QUARTERS, all_but_last)

    def finish(i, total, w):
        a, h, _, _ = split(i)
        wait(land2.at[2, a, h, :, pl.ds(w * rows, rows)], last.at[a, h, w])

        def piece(j, total):
            at = (a, h, j, pl.ds(w * rows, rows))
            g = (partial[at] + land2[(2, *at)].astype(F32)).astype(BF16)
            grads[at] = g
            g = g.astype(F32)
            return total + jnp.sum((g * g).reshape(rows // TILE, TILE, LANES), axis=0)

        return lax.fori_loop(0, layers, piece, total)

    total = jnp.zeros((TILE, LANES), F32)
    for w in range(kinds):
        total = lax.fori_loop(0, QUARTERS, functools.partial(finish, w=w), total)
    squares[me] = jnp.sum(total, axis=0, keepdims=True)

    wait(land1, sent1)
    wait(land2, sent2)

    def far(place):
        return -min(place[0], side - place[0]) - min(place[1], side - place[1])

    for dx, dy, dc in sorted(itertools.product(range(side), range(side), range(CORES)), key=far):
        if not (dx or dy or dc):
            continue
        to = (wrap(x + dx) * side + wrap(y + dy)) * CORES + (core if dc == 0 else 1 - core)
        remote(squares.at[me], squares.at[me], square_sent, square_came, to).start()
    for i, ref in enumerate((w_own, m_own, v_own)):
        wait(ref, state_sem.at[i])
    wait(squares.at[pl.ds(0, n - 1)], square_came)
    total = jnp.sum(jnp.sum(squares[...], axis=0), axis=1, keepdims=True)
    count = n * layers * kinds * QUARTERS * rows * LANES
    factor = jnp.minimum(1.0, 0.5 * lax.rsqrt(total / count + 1e-30))

    def out2(i, d, e, k, far=1):
        a, h, p, q = split(i)
        ref = whole.at[0, a, h, d, :, e]
        remote(ref, ref, out_sent2, arrivals.at[a, h, far * side + e], device(a, wrap(p + k), q)).start()

    def out1(i, e, k):
        a, h, p, q = split(i)
        ref = whole.at[0, a, h, p, :, e]
        remote(ref, ref, out_sent1, arrivals.at[a, h, e], device(a, p, wrap(q + k))).start()

    def pair(i, d, e):
        a, h, _, _ = split(i)
        remote(whole.at[0, a, h, d, :, e], whole.at[1, a, h, d, :, e], pair_sent, pair_came, sibling).start()

    def arrived(i, e, far):
        a, h, _, _ = split(i)
        wait(land2.at[0, 0] if far == 1 else land2.at[0, 0, 0], arrivals.at[a, h, far * side + e])

    def stepped(i, j):
        a, h, _, _ = split(i)
        layer, w = j // kinds, j % kinds
        at = (w, layer, pl.ds(pl.multiple_of(i * rows, rows), rows))
        g = grads[a, h, layer, quarter(w)].astype(F32) * factor
        return at, 0.9 * m_own[at] + 0.1 * g, 0.95 * v_own[at] + 0.05 * g * g

    def update(i, w):
        a, h, p, q = split(i)

        def layer(j):
            at, m, v = stepped(i, j * kinds + w)
            w_old = w_own[at].astype(F32)
            step = m * lax.rsqrt(v + 1e-8) + 0.1 * w_old
            whole[0, a, h, p, j, q, pl.ds(w * rows, rows)] = (w_old - 0.02 * step).astype(BF16)

        steps(layers, layer)
        ref = whole.at[0, a, h, p, :, q, pl.ds(w * rows, rows)]
        k = 2 * h - 1
        remote(ref, ref, out_sent1, arrivals.at[a, h, q], device(a, p, wrap(q + k))).start()
        remote(ref, ref, out_sent2, arrivals.at[a, h, side + q], device(a, wrap(p + k), q)).start()

    for w in range(kinds):
        steps(QUARTERS, lambda i: update(i, w))

    def own(i):
        _, h, p, q = split(i)
        out1(i, q, 1 - 2 * h)
        out2(i, p, q, 1 - 2 * h)
        pair(i, p, q)

    steps(QUARTERS, own)

    def keep(i):
        def piece(j):
            at, m, v = stepped(i, j)
            moments[(0, *at)] = m
            moments[(1, *at)] = v

        steps(layers * kinds, piece)

    steps(QUARTERS, keep)

    def place(r, h):
        return (0, 1 - 2 * h, 2 * h - 1, 2)[r]

    def column(r):
        def run(i):
            _, h, p, q = split(i)
            e = wrap(q + place(r, h))
            arrived(i, e, 0)
            if r == 1:
                out1(i, e, 2 * h - 1)
            out2(i, p, e, 2 * h - 1)
            out2(i, p, e, 1 - 2 * h)
            pair(i, p, e)

        steps(QUARTERS, run)

    def beside(r):
        def run(i):
            a, h, p, q = split(i)
            e = wrap(q + place(r, h))
            d = wrap(p + 1 - 2 * h)
            arrived(i, e, 1)
            if r < 3:
                out2(i, d, e, 2 * h - 1, 2)
            else:
                for w in range(kinds):
                    ref = whole.at[0, a, h, d, :, e, pl.ds(w * rows, rows)]
                    remote(ref, ref, out_sent2, last.at[a, h, w], device(a, wrap(p + 2 * h - 1), q)).start()
            pair(i, d, e)
            pair(i, wrap(p + 2 * h - 1), e)

        steps(QUARTERS, run)

    def across(r):
        def run(i):
            _, h, p, q = split(i)
            e = wrap(q + place(r, h))
            arrived(i, e, 2)
            pair(i, wrap(p + 2), e)

        steps(QUARTERS, run)

    def across_last(i, w):
        a, h, p, q = split(i)
        at = (a, h, wrap(p + 2), slice(None), wrap(q + place(3, h)), pl.ds(w * rows, rows))
        wait(land2.at[0, 0, 0, :, pl.ds(0, rows)], last.at[a, h, w])
        remote(whole.at[(0, *at)], whole.at[(1, *at)], pair_sent, pair_came, sibling).start()

    column(1)
    column(2)
    beside(0)
    column(3)
    beside(1)
    beside(2)
    across(0)
    beside(3)
    across(1)
    across(2)
    for w in range(kinds):
        steps(QUARTERS, lambda i: across_last(i, w))

    wait(whole.at[1], pair_came)
    wait(whole.at[0], pair_sent)
    wait(land1, out_sent2)
    wait(land2, out_sent1)
    wait(whole.at[1], swap_sent)
    wait(squares.at[pl.ds(0, n - 1)], square_sent)


def write_kernel(side, whole, moments, *refs):
    w_refs, m_refs, v_refs, sem = refs[:3], refs[3:6], refs[6:9], refs[9]
    kinds = len(w_refs)
    rows = w_refs[0].shape[-2] // QUARTERS
    core = lax.rem(lax.axis_index("dp"), CORES)

    def copies(d):
        for k in range(CORES):
            c = core if k == 0 else 1 - core
            for a in range(AXES):
                for h in range(HALVES):
                    lines = pl.ds((a * HALVES + h) * rows, rows)
                    for w in range(kinds):
                        dst = w_refs[w].at[:, d, :, c, lines, :] if a == 0 else w_refs[w].at[:, :, d, c, lines, :]
                        pltpu.make_async_copy(whole.at[k, a, h, d, :, :, pl.ds(w * rows, rows), :], dst, sem.at[0]).start()

    steps(side, copies)
    for w in range(kinds):
        pltpu.make_async_copy(moments.at[0, w], m_refs[w], sem.at[1]).start()
        pltpu.make_async_copy(moments.at[1, w], v_refs[w], sem.at[1]).start()
    pltpu.make_async_copy(whole, whole, sem.at[0]).wait()
    pltpu.make_async_copy(moments, moments, sem.at[1]).wait()


def solution(mesh):
    n = mesh.shape["dp"]
    side = math.isqrt(n // CORES)

    def step(*arrays):
        terms, weights, m, v = (arrays[i : i + 3] for i in (0, 3, 6, 9))
        kinds, layers = len(weights), weights[0].shape[0]
        g = [tiled(t[0], side, side, CORES) for t in terms]
        w = [tiled(a, side, side, CORES) for a in weights]
        states = [tiled(a) for a in (*m, *v)]
        block = g[0].shape[-2]
        rows = block // QUARTERS
        unit = kinds * rows
        hbm, vmem = pl.BlockSpec(memory_space=pltpu.HBM), pl.BlockSpec(memory_space=pltpu.VMEM)
        dma = pltpu.SemaphoreType.DMA
        piece = (AXES, HALVES)
        whole, moments = pl.pallas_call(
            functools.partial(exchange_kernel, n, side),
            out_shape=(
                pltpu.VMEM((CORES, *piece, side, layers, side, unit, LANES), BF16),
                pltpu.VMEM((2, kinds, layers, block, LANES), F32),
            ),
            in_specs=[hbm] * 12,
            out_specs=(vmem, vmem),
            scratch_shapes=[
                pltpu.VMEM((3, *piece, side, layers, unit, LANES), BF16),
                pltpu.VMEM((3, *piece, layers, unit, LANES), BF16),
                pltpu.VMEM((*piece, layers, unit, LANES), F32),
                pltpu.VMEM((*piece, layers, unit, LANES), BF16),
                pltpu.VMEM((kinds, layers, block, LANES), BF16),
                pltpu.VMEM((kinds, layers, block, LANES), F32),
                pltpu.VMEM((kinds, layers, block, LANES), F32),
                pltpu.VMEM((n, 1, LANES), F32),
            ],
            compiler_params=pltpu.CompilerParams(collective_id=0, has_side_effects=True, vmem_limit_bytes=33 << 20),
            name="exchange",
        )(*g, *w, *states)
        out = pl.pallas_call(
            functools.partial(write_kernel, side),
            out_shape=tuple(jax.ShapeDtypeStruct(a.shape, a.dtype) for a in (*w, *states)),
            in_specs=[vmem] * 2,
            out_specs=(hbm,) * 9,
            scratch_shapes=[dma((2,))],
            compiler_params=pltpu.CompilerParams(vmem_limit_bytes=1 << 20),
            name="write",
        )(*(pltpu.with_memory_space_constraint(a, pltpu.VMEM) for a in (whole, moments)))
        return tuple(untiled(o, a.shape) for o, a in zip(out, (*weights, *m, *v), strict=True))

    all_of, cut = P(None, None, None), P(None, "dp", None)
    return jax.shard_map(
        step,
        mesh=mesh,
        in_specs=(P(("rep", "dp"), None, None, None),) * 3 + (all_of,) * 3 + (cut,) * 6,
        out_specs=(P("rep", None, None),) * 3 + (P("rep", "dp", None),) * 6,
        check_vma=False,
    )
```

```python
import functools
import itertools
import math

import jax
import jax.numpy as jnp
from jax import lax
from jax.experimental import pallas as pl
from jax.experimental.pallas import tpu as pltpu
from jax.sharding import PartitionSpec as P

LANES = 128
TILE = 8
KINDS = 3
CORES = 2
AXES = 2
HALVES = 2
QUARTERS = AXES * HALVES
F32, BF16 = jnp.float32, jnp.bfloat16


def tiled(a, *blocks):
    layers, rows, columns = a.shape
    a = a.reshape(layers, rows // TILE, TILE, columns // LANES, LANES).transpose(0, 1, 3, 2, 4)
    return a.reshape(layers, *blocks, rows * columns // (LANES * math.prod(blocks)), LANES)


def untiled(a, shape):
    layers, rows, columns = shape
    a = a.reshape(layers, rows // TILE, columns // LANES, TILE, LANES).transpose(0, 1, 3, 2, 4)
    return a.reshape(shape)


def steps(count, body):
    def run(i, carry):
        body(i)
        return carry

    lax.fori_loop(0, count, run, 0)


def exchange_kernel(n, side, *refs):
    kinds, layers, dma, piece = KINDS, refs[0].shape[0], pltpu.SemaphoreType.DMA, (AXES, HALVES)
    pl.run_scoped(
        lambda *sems: exchange(n, side, *refs, *sems),
        dma((4,)),
        dma((3,)),
        dma((QUARTERS, layers, kinds)),
        dma((3,)),
        dma((3,)),
        dma((*piece, 3 * side)),
        dma((*piece, layers, kinds)),
        dma((3,)),
        dma((9,)),
    )


def exchange(n, side, *refs):
    g_refs, w_refs, m_refs, v_refs = (refs[i : i + 3] for i in (0, 3, 6, 9))
    whole, moments = refs[12:14]
    land1, land2, partial, grads, w_own, m_own, v_own, squares = refs[14:22]
    load_first, load_sem, swap_first, swap_next, swap_rest, arrivals, last, state_sem, sent = refs[22:]
    swap_sent, sent1, sent2, square_sent, square_came, out_sent1, out_sent2, pair_sent, pair_came = (sent.at[i] for i in range(9))
    kinds = len(g_refs)
    layers = g_refs[0].shape[0]
    rows = g_refs[0].shape[-2] // QUARTERS
    unit = kinds * rows

    me = lax.axis_index("dp")
    core = lax.rem(me, CORES)
    here = (lax.div(lax.div(me, CORES), side), lax.rem(lax.div(me, CORES), side))
    sibling = me + 1 - 2 * core

    def wrap(i):
        return lax.rem(i + 2 * side, side)

    def split(i):
        a, h = i // HALVES, i % HALVES
        return a, h, (1 - a) * here[0] + a * here[1], (1 - a) * here[1] + a * here[0]

    def chip(a, d, e):
        return (1 - a) * d + a * e, (1 - a) * e + a * d

    def device(a, d, e):
        x, y = chip(a, d, e)
        return (x * side + y) * CORES + core

    def remote(src, dst, send, recv, to):
        return pltpu.make_async_remote_copy(
            src_ref=src, dst_ref=dst, send_sem=send, recv_sem=recv, device_id={"dp": to}, device_id_type=pl.DeviceIdType.MESH
        )

    def quarter(i):
        return pl.ds(pl.multiple_of(i * rows, rows), rows)

    def away(s, h):
        return (2, 1 - 2 * h, 2 * h - 1, 0)[s]

    def wait(ref, sem):
        pltpu.make_async_copy(ref, ref, sem).wait()

    barrier = pltpu.get_barrier_semaphore()
    x, y = here
    beside_me = [sibling] + [device(0, wrap(x + i), wrap(y + j)) for i, j in ((1, 0), (-1, 0), (0, 1), (0, -1))]
    for to in beside_me:
        pl.semaphore_signal(barrier, inc=1, device_id={"dp": to}, device_id_type=pl.DeviceIdType.MESH)

    quarters = [(a, h) for a in range(AXES) for h in range(HALVES)]

    def blocks(of, kind, a, h, w):
        lines = pl.ds((a * HALVES + h) * rows, rows)
        d = wrap(here[a] + away(kind, h))
        src = g_refs[w].at[:, d, :, of, lines, :] if a == 0 else g_refs[w].at[:, :, d, of, lines, :]
        return src, (a, h, d, slice(None), slice(None), pl.ds(w * rows, rows), slice(None))

    def load(kind):
        for a, h in quarters:
            for w in range(kinds):
                src, at = blocks(core, kind, a, h, w)
                pltpu.make_async_copy(src, whole.at[(0, *at)], load_sem.at[kind - 1]).start()

    def state_copies():
        mine = (slice(None), here[0], here[1], core)
        for w in range(kinds):
            yield pltpu.make_async_copy(w_refs[w].at[mine], w_own.at[w], state_sem.at[0])
            yield pltpu.make_async_copy(m_refs[w], m_own.at[w], state_sem.at[1])
            yield pltpu.make_async_copy(v_refs[w], v_own.at[w], state_sem.at[2])

    pieces = list(itertools.product(range(layers), range(kinds)))

    def across_at(i, s, w, of, layer=slice(None)):
        a, h, p, q = split(i)
        d, e = wrap(p + 2), wrap(q + away(s, h))
        return g_refs[w].at[(layer, *chip(a, d, e), of, quarter(i), slice(None))], (a, h, d, layer, e, pl.ds(w * rows, rows))

    def load_across(s):
        def one(i):
            for w in range(kinds):
                src, at = across_at(i, s, w, core)
                pltpu.make_async_copy(src, whole.at[(0, *at)], load_first.at[s]).start()

        steps(QUARTERS, one)

    load_across(0)
    pl.semaphore_wait(barrier, len(beside_me))

    def swap_one(i, s, w, sem, layer=slice(None)):
        src, at = across_at(i, s, w, 1 - core, layer)
        remote(src, whole.at[(1, *at)], swap_sent, sem, sibling).start()

    def swap_across(s):
        def one(i):
            for w in range(kinds):
                swap_one(i, s, w, swap_next.at[s - 1])

        steps(QUARTERS, one)

    def swap(kind):
        for a, h in quarters:
            for w in range(kinds):
                src, at = blocks(1 - core, kind, a, h, w)
                remote(src, whole.at[(1, *at)], swap_sent, swap_rest.at[kind - 1], sibling).start()

    for layer, w in pieces:
        steps(QUARTERS, lambda i: swap_one(i, 0, w, swap_first.at[i, layer, w], layer))
    load_across(1)
    swap_across(1)

    def wait_load(kind):
        wait(whole.at[0, :, :, 0], load_sem.at[kind - 1])

    def wait_swap(kind):
        wait(whole.at[1, :, :, 0], swap_rest.at[kind - 1])

    def add(dst, *srcs):
        def piece(j):
            at = (j // kinds, quarter(j % kinds))
            total = srcs[0][at].astype(F32)
            for src in srcs[1:]:
                total += src[at].astype(F32)
            dst[at] = total.astype(BF16)

        steps(layers * kinds, piece)

    def toward(kind, p, h):
        return wrap(p + (2 * h - 1, 1 - 2 * h, 2 * h - 1)[kind])

    def arrival1(kind, a, h, s):
        return arrivals.at[a, h, (s, 8, 4 + s)[kind]]

    def pass1(kind, i, s):
        a, h, p, q = split(i)
        d, e = wrap(p + away(kind, h)), wrap(q + away(s, h))
        terms, others = whole.at[0, a, h, d, :, e], whole.at[1, a, h, d, :, e]
        to = device(a, toward(kind, p, h), q)
        return terms, others, remote(terms, land1.at[kind, a, h, s], sent1, arrival1(kind, a, h, s), to)

    a_piece = land2.at[0, 0, 0, 0, pl.ds(0, rows)]

    def across_piece(i, layer, w):
        a, h, p, q = split(i)
        d, e = wrap(p + 2), wrap(q + away(0, h))
        own, other = (whole.at[k, a, h, d, layer, e, pl.ds(w * rows, rows)] for k in range(2))
        wait(a_piece, swap_first.at[i, layer, w])
        own[...] = (own[...].astype(F32) + other[...].astype(F32)).astype(BF16)
        to = device(a, toward(0, p, h), q)
        remote(own, land1.at[0, a, h, 0, layer, pl.ds(w * rows, rows)], sent1, arrival1(0, a, h, 0), to).start()

    for s in range(4):
        wait(land2.at[0], load_first.at[s])
        if s == 0:
            for layer, w in pieces:
                steps(QUARTERS, lambda i: across_piece(i, layer, w))
        else:
            wait(land2.at[0], swap_next.at[s - 1])

            def across_first(i):
                terms, others, copy = pass1(0, i, s)
                add(terms, terms, others)
                copy.start()

            steps(QUARTERS, across_first)
        if s == 0:
            load_across(2)
            swap_across(2)
            load_across(3)
            swap_across(3)
            load(1)
        if s == 1:
            swap(1)
            load(2)
        if s == 2:
            swap(2)
            load(3)
            swap(3)

    for kind in (1, 2):
        wait_load(kind)
        wait_swap(kind)
        for s in range(4):

            def start1(i):
                a, h, _, _ = split(i)
                terms, others, copy = pass1(kind, i, s)
                if kind == 2:
                    wait(land1.at[0, a, h, s], arrival1(0, a, h, s))
                    add(terms, terms, others, land1.at[0, a, h, s])
                else:
                    add(terms, terms, others)
                copy.start()

            steps(QUARTERS, start1)

    for copy in state_copies():
        copy.start()

    def arrival2(kind, a, h):
        return arrivals.at[a, h, 9 + kind]

    def pass2(kind, i):
        a, h, p, q = split(i)
        e = wrap(q + away(kind, h))
        terms, to = whole.at[0, a, h, p, :, e], device(a, p, toward(kind, q, h))
        if kind < 2:
            return [remote(terms, land2.at[kind, a, h], sent2, arrival2(kind, a, h), to)]
        parts = [(layer, pl.ds(w * rows, rows), last.at[a, h, layer, w]) for layer, w in pieces]
        return [remote(terms.at[layer, at], land2.at[kind, a, h, layer, at], sent2, sem, to) for layer, at, sem in parts]

    wait_load(3)
    wait_swap(3)
    for kind in range(3):

        def start2(i):
            a, h, p, q = split(i)
            e = wrap(q + away(kind, h))
            if kind == 0:
                wait(land1.at[1, a, h], arrival1(1, a, h, 0))
            wait(land1.at[2, a, h, kind], arrival1(2, a, h, kind))
            terms = whole.at[0, a, h, p, :, e]
            srcs = [terms, whole.at[1, a, h, p, :, e], land1.at[1, a, h, kind], land1.at[2, a, h, kind]]
            if kind == 2:
                wait(land2.at[0, a, h], arrival2(0, a, h))
                srcs.append(land2.at[0, a, h])
            add(terms, *srcs)
            for copy in pass2(kind, i):
                copy.start()

        steps(QUARTERS, start2)

    def all_but_last(i):
        a, h, p, q = split(i)
        wait(land1.at[2, a, h, 3], arrival1(2, a, h, 3))
        wait(land2.at[1, a, h], arrival2(1, a, h))
        srcs = [whole.at[k, a, h, p, :, q] for k in range(2)] + [land1.at[k, a, h, 3] for k in (1, 2)] + [land2.at[1, a, h]]

        def piece(j):
            at = (j // kinds, quarter(j % kinds))
            partial[(a, h, *at)] = sum(src[at].astype(F32) for src in srcs)

        steps(layers * kinds, piece)

    steps(QUARTERS, all_but_last)

    def finish(i, total, layer, w):
        a, h, _, _ = split(i)
        wait(a_piece, last.at[a, h, layer, w])
        at = (a, h, layer, pl.ds(w * rows, rows))
        g = (partial[at] + land2[(2, *at)].astype(F32)).astype(BF16)
        grads[at] = g
        g = g.astype(F32)
        return total + jnp.sum((g * g).reshape(rows // TILE, TILE, LANES), axis=0)

    total = jnp.zeros((TILE, LANES), F32)
    for layer, w in pieces:
        total = lax.fori_loop(0, QUARTERS, functools.partial(finish, layer=layer, w=w), total)
    squares[me] = jnp.sum(total, axis=0, keepdims=True)

    wait(land1, sent1)
    wait(land2, sent2)

    def far(place):
        return -min(place[0], side - place[0]) - min(place[1], side - place[1])

    for dx, dy, dc in sorted(itertools.product(range(side), range(side), range(CORES)), key=far):
        if not (dx or dy or dc):
            continue
        to = (wrap(x + dx) * side + wrap(y + dy)) * CORES + (core if dc == 0 else 1 - core)
        remote(squares.at[me], squares.at[me], square_sent, square_came, to).start()
    for i, ref in enumerate((w_own, m_own, v_own)):
        wait(ref, state_sem.at[i])
    wait(squares.at[pl.ds(0, n - 1)], square_came)
    total = jnp.sum(jnp.sum(squares[...], axis=0), axis=1, keepdims=True)
    count = n * layers * kinds * QUARTERS * rows * LANES
    factor = jnp.minimum(1.0, 0.5 * lax.rsqrt(total / count + 1e-30))

    def out2(i, d, e, k, far=1):
        a, h, p, q = split(i)
        ref = whole.at[0, a, h, d, :, e]
        remote(ref, ref, out_sent2, arrivals.at[a, h, far * side + e], device(a, wrap(p + k), q)).start()

    def out1(i, e, k):
        a, h, p, q = split(i)
        ref = whole.at[0, a, h, p, :, e]
        remote(ref, ref, out_sent1, arrivals.at[a, h, e], device(a, p, wrap(q + k))).start()

    def pair(i, d, e):
        a, h, _, _ = split(i)
        remote(whole.at[0, a, h, d, :, e], whole.at[1, a, h, d, :, e], pair_sent, pair_came, sibling).start()

    def arrived(i, e, far):
        a, h, _, _ = split(i)
        wait(land2.at[0, 0] if far == 1 else land2.at[0, 0, 0], arrivals.at[a, h, far * side + e])

    def stepped(i, j):
        a, h, _, _ = split(i)
        layer, w = j // kinds, j % kinds
        at = (w, layer, pl.ds(pl.multiple_of(i * rows, rows), rows))
        g = grads[a, h, layer, quarter(w)].astype(F32) * factor
        return at, 0.9 * m_own[at] + 0.1 * g, 0.95 * v_own[at] + 0.05 * g * g

    def update(i, layer, w):
        a, h, p, q = split(i)
        at, m, v = stepped(i, layer * kinds + w)
        w_old = w_own[at].astype(F32)
        step = m * lax.rsqrt(v + 1e-8) + 0.1 * w_old
        ref = whole.at[0, a, h, p, layer, q, pl.ds(w * rows, rows)]
        ref[...] = (w_old - 0.02 * step).astype(BF16)
        k = 2 * h - 1
        remote(ref, ref, out_sent1, arrivals.at[a, h, q], device(a, p, wrap(q + k))).start()
        remote(ref, ref, out_sent2, arrivals.at[a, h, side + q], device(a, wrap(p + k), q)).start()

    for layer, w in pieces:
        steps(QUARTERS, lambda i: update(i, layer, w))

    def own(i):
        _, h, p, q = split(i)
        out1(i, q, 1 - 2 * h)
        out2(i, p, q, 1 - 2 * h)
        pair(i, p, q)

    steps(QUARTERS, own)

    def keep(i):
        def piece(j):
            at, m, v = stepped(i, j)
            moments[(0, *at)] = m
            moments[(1, *at)] = v

        steps(layers * kinds, piece)

    steps(QUARTERS, keep)

    def place(r, h):
        return (0, 1 - 2 * h, 2 * h - 1, 2)[r]

    def column(r):
        def run(i):
            _, h, p, q = split(i)
            e = wrap(q + place(r, h))
            arrived(i, e, 0)
            if r == 1:
                out1(i, e, 2 * h - 1)
            out2(i, p, e, 2 * h - 1)
            out2(i, p, e, 1 - 2 * h)
            pair(i, p, e)

        steps(QUARTERS, run)

    def beside(r):
        def run(i):
            a, h, p, q = split(i)
            e = wrap(q + place(r, h))
            d = wrap(p + 1 - 2 * h)
            arrived(i, e, 1)
            if r < 3:
                out2(i, d, e, 2 * h - 1, 2)
            else:
                for layer, w in pieces:
                    ref = whole.at[0, a, h, d, layer, e, pl.ds(w * rows, rows)]
                    remote(ref, ref, out_sent2, last.at[a, h, layer, w], device(a, wrap(p + 2 * h - 1), q)).start()
            pair(i, d, e)
            pair(i, wrap(p + 2 * h - 1), e)

        steps(QUARTERS, run)

    def across(r):
        def run(i):
            _, h, p, q = split(i)
            e = wrap(q + place(r, h))
            arrived(i, e, 2)
            pair(i, wrap(p + 2), e)

        steps(QUARTERS, run)

    def across_last(i, layer, w):
        a, h, p, q = split(i)
        at = (a, h, wrap(p + 2), layer, wrap(q + place(3, h)), pl.ds(w * rows, rows))
        wait(a_piece, last.at[a, h, layer, w])
        remote(whole.at[(0, *at)], whole.at[(1, *at)], pair_sent, pair_came, sibling).start()

    column(1)
    column(2)
    beside(0)
    column(3)
    beside(1)
    beside(2)
    across(0)
    beside(3)
    across(1)
    across(2)
    for layer, w in pieces:
        steps(QUARTERS, lambda i: across_last(i, layer, w))

    wait(whole.at[1], pair_came)
    wait(whole.at[0], pair_sent)
    wait(land1, out_sent2)
    wait(land2, out_sent1)
    wait(whole.at[1], swap_sent)
    wait(squares.at[pl.ds(0, n - 1)], square_sent)


def write_kernel(side, whole, moments, *refs):
    w_refs, m_refs, v_refs, sem = refs[:3], refs[3:6], refs[6:9], refs[9]
    kinds = len(w_refs)
    rows = w_refs[0].shape[-2] // QUARTERS
    core = lax.rem(lax.axis_index("dp"), CORES)

    def copies(d):
        for k in range(CORES):
            c = core if k == 0 else 1 - core
            for a in range(AXES):
                for h in range(HALVES):
                    lines = pl.ds((a * HALVES + h) * rows, rows)
                    for w in range(kinds):
                        dst = w_refs[w].at[:, d, :, c, lines, :] if a == 0 else w_refs[w].at[:, :, d, c, lines, :]
                        pltpu.make_async_copy(whole.at[k, a, h, d, :, :, pl.ds(w * rows, rows), :], dst, sem.at[0]).start()

    steps(side, copies)
    for w in range(kinds):
        pltpu.make_async_copy(moments.at[0, w], m_refs[w], sem.at[1]).start()
        pltpu.make_async_copy(moments.at[1, w], v_refs[w], sem.at[1]).start()
    pltpu.make_async_copy(whole, whole, sem.at[0]).wait()
    pltpu.make_async_copy(moments, moments, sem.at[1]).wait()


def solution(mesh):
    n = mesh.shape["dp"]
    side = math.isqrt(n // CORES)

    def step(*arrays):
        terms, weights, m, v = (arrays[i : i + 3] for i in (0, 3, 6, 9))
        kinds, layers = len(weights), weights[0].shape[0]
        g = [tiled(t[0], side, side, CORES) for t in terms]
        w = [tiled(a, side, side, CORES) for a in weights]
        states = [tiled(a) for a in (*m, *v)]
        block = g[0].shape[-2]
        rows = block // QUARTERS
        unit = kinds * rows
        hbm, vmem = pl.BlockSpec(memory_space=pltpu.HBM), pl.BlockSpec(memory_space=pltpu.VMEM)
        dma = pltpu.SemaphoreType.DMA
        piece = (AXES, HALVES)
        whole, moments = pl.pallas_call(
            functools.partial(exchange_kernel, n, side),
            out_shape=(
                pltpu.VMEM((CORES, *piece, side, layers, side, unit, LANES), BF16),
                pltpu.VMEM((2, kinds, layers, block, LANES), F32),
            ),
            in_specs=[hbm] * 12,
            out_specs=(vmem, vmem),
            scratch_shapes=[
                pltpu.VMEM((3, *piece, side, layers, unit, LANES), BF16),
                pltpu.VMEM((3, *piece, layers, unit, LANES), BF16),
                pltpu.VMEM((*piece, layers, unit, LANES), F32),
                pltpu.VMEM((*piece, layers, unit, LANES), BF16),
                pltpu.VMEM((kinds, layers, block, LANES), BF16),
                pltpu.VMEM((kinds, layers, block, LANES), F32),
                pltpu.VMEM((kinds, layers, block, LANES), F32),
                pltpu.VMEM((n, 1, LANES), F32),
            ],
            compiler_params=pltpu.CompilerParams(collective_id=0, has_side_effects=True, vmem_limit_bytes=33 << 20),
            name="exchange",
        )(*g, *w, *states)
        out = pl.pallas_call(
            functools.partial(write_kernel, side),
            out_shape=tuple(jax.ShapeDtypeStruct(a.shape, a.dtype) for a in (*w, *states)),
            in_specs=[vmem] * 2,
            out_specs=(hbm,) * 9,
            scratch_shapes=[dma((2,))],
            compiler_params=pltpu.CompilerParams(vmem_limit_bytes=1 << 20),
            name="write",
        )(*(pltpu.with_memory_space_constraint(a, pltpu.VMEM) for a in (whole, moments)))
        return tuple(untiled(o, a.shape) for o, a in zip(out, (*weights, *m, *v), strict=True))

    all_of, cut = P(None, None, None), P(None, "dp", None)
    return jax.shard_map(
        step,
        mesh=mesh,
        in_specs=(P(("rep", "dp"), None, None, None),) * 3 + (all_of,) * 3 + (cut,) * 6,
        out_specs=(P("rep", None, None),) * 3 + (P("rep", "dp", None),) * 6,
        check_vma=False,
    )
```

```python
import functools
import itertools
import math

import jax
import jax.numpy as jnp
from jax import lax
from jax.experimental import pallas as pl
from jax.experimental.pallas import tpu as pltpu
from jax.sharding import PartitionSpec as P

LANES = 128
TILE = 8
KINDS = 3
CORES = 2
AXES = 2
HALVES = 2
QUARTERS = AXES * HALVES
F32, BF16 = jnp.float32, jnp.bfloat16


def tiled(a, *blocks):
    layers, rows, columns = a.shape
    a = a.reshape(layers, rows // TILE, TILE, columns // LANES, LANES).transpose(0, 1, 3, 2, 4)
    return a.reshape(layers, *blocks, rows * columns // (LANES * math.prod(blocks)), LANES)


def untiled(a, shape):
    layers, rows, columns = shape
    a = a.reshape(layers, rows // TILE, columns // LANES, TILE, LANES).transpose(0, 1, 3, 2, 4)
    return a.reshape(shape)


def steps(count, body):
    def run(i, carry):
        body(i)
        return carry

    lax.fori_loop(0, count, run, 0)


def exchange_kernel(n, side, *refs):
    kinds, layers, dma, piece = KINDS, refs[0].shape[0], pltpu.SemaphoreType.DMA, (AXES, HALVES)
    pl.run_scoped(
        lambda *sems: exchange(n, side, *refs, *sems),
        dma((4,)),
        dma((3,)),
        dma((QUARTERS, layers, kinds)),
        dma((3,)),
        dma((3,)),
        dma((*piece, 3 * side)),
        dma((*piece, layers, kinds)),
        dma((3,)),
        dma((9,)),
    )


def exchange(n, side, *refs):
    g_refs, w_refs, m_refs, v_refs = (refs[i : i + 3] for i in (0, 3, 6, 9))
    whole, moments = refs[12:14]
    land1, land2, partial, grads, w_own, m_own, v_own, squares = refs[14:22]
    load_first, load_sem, swap_first, swap_next, swap_rest, arrivals, last, state_sem, sent = refs[22:]
    swap_sent, sent1, sent2, square_sent, square_came, out_sent1, out_sent2, pair_sent, pair_came = (sent.at[i] for i in range(9))
    kinds = len(g_refs)
    layers = g_refs[0].shape[0]
    rows = g_refs[0].shape[-2] // QUARTERS
    unit = kinds * rows

    me = lax.axis_index("dp")
    core = lax.rem(me, CORES)
    here = (lax.div(lax.div(me, CORES), side), lax.rem(lax.div(me, CORES), side))
    sibling = me + 1 - 2 * core

    def wrap(i):
        return lax.rem(i + 2 * side, side)

    def split(i):
        a, h = i // HALVES, i % HALVES
        return a, h, (1 - a) * here[0] + a * here[1], (1 - a) * here[1] + a * here[0]

    def chip(a, d, e):
        return (1 - a) * d + a * e, (1 - a) * e + a * d

    def device(a, d, e):
        x, y = chip(a, d, e)
        return (x * side + y) * CORES + core

    def remote(src, dst, send, recv, to):
        return pltpu.make_async_remote_copy(
            src_ref=src, dst_ref=dst, send_sem=send, recv_sem=recv, device_id={"dp": to}, device_id_type=pl.DeviceIdType.MESH
        )

    def quarter(i):
        return pl.ds(pl.multiple_of(i * rows, rows), rows)

    def away(s, h):
        return (2, 1 - 2 * h, 2 * h - 1, 0)[s]

    def wait(ref, sem):
        pltpu.make_async_copy(ref, ref, sem).wait()

    barrier = pltpu.get_barrier_semaphore()
    x, y = here
    beside_me = [sibling] + [device(0, wrap(x + i), wrap(y + j)) for i, j in ((1, 0), (-1, 0), (0, 1), (0, -1))]
    for to in beside_me:
        pl.semaphore_signal(barrier, inc=1, device_id={"dp": to}, device_id_type=pl.DeviceIdType.MESH)

    quarters = [(a, h) for a in range(AXES) for h in range(HALVES)]

    def blocks(of, kind, a, h, w):
        lines = pl.ds((a * HALVES + h) * rows, rows)
        d = wrap(here[a] + away(kind, h))
        src = g_refs[w].at[:, d, :, of, lines, :] if a == 0 else g_refs[w].at[:, :, d, of, lines, :]
        return src, (a, h, d, slice(None), slice(None), pl.ds(w * rows, rows), slice(None))

    def load(kind):
        for a, h in quarters:
            for w in range(kinds):
                src, at = blocks(core, kind, a, h, w)
                pltpu.make_async_copy(src, whole.at[(0, *at)], load_sem.at[kind - 1]).start()

    def state_copies():
        mine = (slice(None), here[0], here[1], core)
        for w in range(kinds):
            yield pltpu.make_async_copy(w_refs[w].at[mine], w_own.at[w], state_sem.at[0])
            yield pltpu.make_async_copy(m_refs[w], m_own.at[w], state_sem.at[1])
            yield pltpu.make_async_copy(v_refs[w], v_own.at[w], state_sem.at[2])

    pieces = list(itertools.product(range(layers), range(kinds)))

    def across_at(i, s, w, of, layer=slice(None)):
        a, h, p, q = split(i)
        d, e = wrap(p + 2), wrap(q + away(s, h))
        return g_refs[w].at[(layer, *chip(a, d, e), of, quarter(i), slice(None))], (a, h, d, layer, e, pl.ds(w * rows, rows))

    def load_across(s):
        def one(i):
            for w in range(kinds):
                src, at = across_at(i, s, w, core)
                pltpu.make_async_copy(src, whole.at[(0, *at)], load_first.at[s]).start()

        steps(QUARTERS, one)

    load_across(0)
    pl.semaphore_wait(barrier, len(beside_me))

    def swap_one(i, s, w, sem, layer=slice(None)):
        src, at = across_at(i, s, w, 1 - core, layer)
        remote(src, whole.at[(1, *at)], swap_sent, sem, sibling).start()

    def swap_across(s):
        def one(i):
            for w in range(kinds):
                swap_one(i, s, w, swap_next.at[s - 1])

        steps(QUARTERS, one)

    def swap(kind):
        for a, h in quarters:
            for w in range(kinds):
                src, at = blocks(1 - core, kind, a, h, w)
                remote(src, whole.at[(1, *at)], swap_sent, swap_rest.at[kind - 1], sibling).start()

    for layer, w in pieces:
        steps(QUARTERS, lambda i: swap_one(i, 0, w, swap_first.at[i, layer, w], layer))

    def wait_load(kind):
        wait(whole.at[0, :, :, 0], load_sem.at[kind - 1])

    def wait_swap(kind):
        wait(whole.at[1, :, :, 0], swap_rest.at[kind - 1])

    def add(dst, *srcs):
        def piece(j):
            at = (j // kinds, quarter(j % kinds))
            total = srcs[0][at].astype(F32)
            for src in srcs[1:]:
                total += src[at].astype(F32)
            dst[at] = total.astype(BF16)

        steps(layers * kinds, piece)

    def toward(kind, p, h):
        return wrap(p + (2 * h - 1, 1 - 2 * h, 2 * h - 1)[kind])

    def arrival1(kind, a, h, s):
        return arrivals.at[a, h, (s, 8, 4 + s)[kind]]

    def pass1(kind, i, s):
        a, h, p, q = split(i)
        d, e = wrap(p + away(kind, h)), wrap(q + away(s, h))
        terms, others = whole.at[0, a, h, d, :, e], whole.at[1, a, h, d, :, e]
        to = device(a, toward(kind, p, h), q)
        return terms, others, remote(terms, land1.at[kind, a, h, s], sent1, arrival1(kind, a, h, s), to)

    a_piece = land2.at[0, 0, 0, 0, pl.ds(0, rows)]

    def across_piece(i, layer, w):
        a, h, p, q = split(i)
        d, e = wrap(p + 2), wrap(q + away(0, h))
        own, other = (whole.at[k, a, h, d, layer, e, pl.ds(w * rows, rows)] for k in range(2))
        wait(a_piece, swap_first.at[i, layer, w])
        own[...] = (own[...].astype(F32) + other[...].astype(F32)).astype(BF16)
        to = device(a, toward(0, p, h), q)
        remote(own, land1.at[0, a, h, 0, layer, pl.ds(w * rows, rows)], sent1, arrival1(0, a, h, 0), to).start()

    for s in range(4):
        wait(land2.at[0], load_first.at[s])
        if s == 0:
            for layer, w in pieces:
                steps(QUARTERS, lambda i: across_piece(i, layer, w))
        else:
            wait(land2.at[0], swap_next.at[s - 1])

            def across_first(i):
                terms, others, copy = pass1(0, i, s)
                add(terms, terms, others)
                copy.start()

            steps(QUARTERS, across_first)
        if s == 0:
            load_across(1)
            swap_across(1)
            load_across(2)
            swap_across(2)
            load_across(3)
            swap_across(3)
            load(1)
        if s == 1:
            swap(1)
            load(2)
        if s == 2:
            swap(2)
            load(3)
            swap(3)

    for kind in (1, 2):
        wait_load(kind)
        wait_swap(kind)
        for s in range(4):

            def start1(i):
                a, h, _, _ = split(i)
                terms, others, copy = pass1(kind, i, s)
                if kind == 2:
                    wait(land1.at[0, a, h, s], arrival1(0, a, h, s))
                    add(terms, terms, others, land1.at[0, a, h, s])
                else:
                    add(terms, terms, others)
                copy.start()

            steps(QUARTERS, start1)

    for copy in state_copies():
        copy.start()

    def arrival2(kind, a, h):
        return arrivals.at[a, h, 9 + kind]

    def pass2(kind, i):
        a, h, p, q = split(i)
        e = wrap(q + away(kind, h))
        terms, to = whole.at[0, a, h, p, :, e], device(a, p, toward(kind, q, h))
        if kind < 2:
            return [remote(terms, land2.at[kind, a, h], sent2, arrival2(kind, a, h), to)]
        parts = [(layer, pl.ds(w * rows, rows), last.at[a, h, layer, w]) for layer, w in pieces]
        return [remote(terms.at[layer, at], land2.at[kind, a, h, layer, at], sent2, sem, to) for layer, at, sem in parts]

    wait_load(3)
    wait_swap(3)
    for kind in range(3):

        def start2(i):
            a, h, p, q = split(i)
            e = wrap(q + away(kind, h))
            if kind == 0:
                wait(land1.at[1, a, h], arrival1(1, a, h, 0))
            wait(land1.at[2, a, h, kind], arrival1(2, a, h, kind))
            terms = whole.at[0, a, h, p, :, e]
            srcs = [terms, whole.at[1, a, h, p, :, e], land1.at[1, a, h, kind], land1.at[2, a, h, kind]]
            if kind == 2:
                wait(land2.at[0, a, h], arrival2(0, a, h))
                srcs.append(land2.at[0, a, h])
            add(terms, *srcs)
            for copy in pass2(kind, i):
                copy.start()

        steps(QUARTERS, start2)

    def all_but_last(i):
        a, h, p, q = split(i)
        wait(land1.at[2, a, h, 3], arrival1(2, a, h, 3))
        wait(land2.at[1, a, h], arrival2(1, a, h))
        srcs = [whole.at[k, a, h, p, :, q] for k in range(2)] + [land1.at[k, a, h, 3] for k in (1, 2)] + [land2.at[1, a, h]]

        def piece(j):
            at = (j // kinds, quarter(j % kinds))
            partial[(a, h, *at)] = sum(src[at].astype(F32) for src in srcs)

        steps(layers * kinds, piece)

    steps(QUARTERS, all_but_last)

    def finish(i, total, layer, w):
        a, h, _, _ = split(i)
        wait(a_piece, last.at[a, h, layer, w])
        at = (a, h, layer, pl.ds(w * rows, rows))
        g = (partial[at] + land2[(2, *at)].astype(F32)).astype(BF16)
        grads[at] = g
        g = g.astype(F32)
        return total + jnp.sum((g * g).reshape(rows // TILE, TILE, LANES), axis=0)

    total = jnp.zeros((TILE, LANES), F32)
    for layer, w in pieces:
        total = lax.fori_loop(0, QUARTERS, functools.partial(finish, layer=layer, w=w), total)
    squares[me] = jnp.sum(total, axis=0, keepdims=True)

    wait(land1, sent1)
    wait(land2, sent2)

    def far(place):
        return -min(place[0], side - place[0]) - min(place[1], side - place[1])

    for dx, dy, dc in sorted(itertools.product(range(side), range(side), range(CORES)), key=far):
        if not (dx or dy or dc):
            continue
        to = (wrap(x + dx) * side + wrap(y + dy)) * CORES + (core if dc == 0 else 1 - core)
        remote(squares.at[me], squares.at[me], square_sent, square_came, to).start()
    for i, ref in enumerate((w_own, m_own, v_own)):
        wait(ref, state_sem.at[i])
    wait(squares.at[pl.ds(0, n - 1)], square_came)
    total = jnp.sum(jnp.sum(squares[...], axis=0), axis=1, keepdims=True)
    count = n * layers * kinds * QUARTERS * rows * LANES
    factor = jnp.minimum(1.0, 0.5 * lax.rsqrt(total / count + 1e-30))

    def out2(i, d, e, k, far=1):
        a, h, p, q = split(i)
        ref = whole.at[0, a, h, d, :, e]
        remote(ref, ref, out_sent2, arrivals.at[a, h, far * side + e], device(a, wrap(p + k), q)).start()

    def out1(i, e, k):
        a, h, p, q = split(i)
        ref = whole.at[0, a, h, p, :, e]
        remote(ref, ref, out_sent1, arrivals.at[a, h, e], device(a, p, wrap(q + k))).start()

    def pair(i, d, e):
        a, h, _, _ = split(i)
        remote(whole.at[0, a, h, d, :, e], whole.at[1, a, h, d, :, e], pair_sent, pair_came, sibling).start()

    def arrived(i, e, far):
        a, h, _, _ = split(i)
        wait(land2.at[0, 0] if far == 1 else land2.at[0, 0, 0], arrivals.at[a, h, far * side + e])

    def stepped(i, j):
        a, h, _, _ = split(i)
        layer, w = j // kinds, j % kinds
        at = (w, layer, pl.ds(pl.multiple_of(i * rows, rows), rows))
        g = grads[a, h, layer, quarter(w)].astype(F32) * factor
        return at, 0.9 * m_own[at] + 0.1 * g, 0.95 * v_own[at] + 0.05 * g * g

    def update(i, layer, w):
        a, h, p, q = split(i)
        at, m, v = stepped(i, layer * kinds + w)
        w_old = w_own[at].astype(F32)
        step = m * lax.rsqrt(v + 1e-8) + 0.1 * w_old
        ref = whole.at[0, a, h, p, layer, q, pl.ds(w * rows, rows)]
        ref[...] = (w_old - 0.02 * step).astype(BF16)
        k = 2 * h - 1
        remote(ref, ref, out_sent1, arrivals.at[a, h, q], device(a, p, wrap(q + k))).start()
        remote(ref, ref, out_sent2, arrivals.at[a, h, side + q], device(a, wrap(p + k), q)).start()

    for layer, w in pieces:
        steps(QUARTERS, lambda i: update(i, layer, w))

    def own(i):
        _, h, p, q = split(i)
        out1(i, q, 1 - 2 * h)
        out2(i, p, q, 1 - 2 * h)
        pair(i, p, q)

    steps(QUARTERS, own)

    def keep(i):
        def piece(j):
            at, m, v = stepped(i, j)
            moments[(0, *at)] = m
            moments[(1, *at)] = v

        steps(layers * kinds, piece)

    steps(QUARTERS, keep)

    def place(r, h):
        return (0, 1 - 2 * h, 2 * h - 1, 2)[r]

    def column(r):
        def run(i):
            _, h, p, q = split(i)
            e = wrap(q + place(r, h))
            arrived(i, e, 0)
            if r == 1:
                out1(i, e, 2 * h - 1)
            out2(i, p, e, 2 * h - 1)
            out2(i, p, e, 1 - 2 * h)
            pair(i, p, e)

        steps(QUARTERS, run)

    def beside(r):
        def run(i):
            a, h, p, q = split(i)
            e = wrap(q + place(r, h))
            d = wrap(p + 1 - 2 * h)
            arrived(i, e, 1)
            if r < 3:
                out2(i, d, e, 2 * h - 1, 2)
            else:
                for layer, w in pieces:
                    ref = whole.at[0, a, h, d, layer, e, pl.ds(w * rows, rows)]
                    remote(ref, ref, out_sent2, last.at[a, h, layer, w], device(a, wrap(p + 2 * h - 1), q)).start()
            pair(i, d, e)
            pair(i, wrap(p + 2 * h - 1), e)

        steps(QUARTERS, run)

    def across(r):
        def run(i):
            _, h, p, q = split(i)
            e = wrap(q + place(r, h))
            arrived(i, e, 2)
            pair(i, wrap(p + 2), e)

        steps(QUARTERS, run)

    def across_last(i, layer, w):
        a, h, p, q = split(i)
        at = (a, h, wrap(p + 2), layer, wrap(q + place(3, h)), pl.ds(w * rows, rows))
        wait(a_piece, last.at[a, h, layer, w])
        remote(whole.at[(0, *at)], whole.at[(1, *at)], pair_sent, pair_came, sibling).start()

    column(1)
    column(2)
    beside(0)
    column(3)
    beside(1)
    beside(2)
    across(0)
    beside(3)
    across(1)
    across(2)
    for layer, w in pieces:
        steps(QUARTERS, lambda i: across_last(i, layer, w))

    wait(whole.at[1], pair_came)
    wait(whole.at[0], pair_sent)
    wait(land1, out_sent2)
    wait(land2, out_sent1)
    wait(whole.at[1], swap_sent)
    wait(squares.at[pl.ds(0, n - 1)], square_sent)


def write_kernel(side, whole, moments, *refs):
    w_refs, m_refs, v_refs, sem = refs[:3], refs[3:6], refs[6:9], refs[9]
    kinds = len(w_refs)
    rows = w_refs[0].shape[-2] // QUARTERS
    core = lax.rem(lax.axis_index("dp"), CORES)

    def copies(d):
        for k in range(CORES):
            c = core if k == 0 else 1 - core
            for a in range(AXES):
                for h in range(HALVES):
                    lines = pl.ds((a * HALVES + h) * rows, rows)
                    for w in range(kinds):
                        dst = w_refs[w].at[:, d, :, c, lines, :] if a == 0 else w_refs[w].at[:, :, d, c, lines, :]
                        pltpu.make_async_copy(whole.at[k, a, h, d, :, :, pl.ds(w * rows, rows), :], dst, sem.at[0]).start()

    steps(side, copies)
    for w in range(kinds):
        pltpu.make_async_copy(moments.at[0, w], m_refs[w], sem.at[1]).start()
        pltpu.make_async_copy(moments.at[1, w], v_refs[w], sem.at[1]).start()
    pltpu.make_async_copy(whole, whole, sem.at[0]).wait()
    pltpu.make_async_copy(moments, moments, sem.at[1]).wait()


def solution(mesh):
    n = mesh.shape["dp"]
    side = math.isqrt(n // CORES)

    def step(*arrays):
        terms, weights, m, v = (arrays[i : i + 3] for i in (0, 3, 6, 9))
        kinds, layers = len(weights), weights[0].shape[0]
        g = [tiled(t[0], side, side, CORES) for t in terms]
        w = [tiled(a, side, side, CORES) for a in weights]
        states = [tiled(a) for a in (*m, *v)]
        block = g[0].shape[-2]
        rows = block // QUARTERS
        unit = kinds * rows
        hbm, vmem = pl.BlockSpec(memory_space=pltpu.HBM), pl.BlockSpec(memory_space=pltpu.VMEM)
        dma = pltpu.SemaphoreType.DMA
        piece = (AXES, HALVES)
        whole, moments = pl.pallas_call(
            functools.partial(exchange_kernel, n, side),
            out_shape=(
                pltpu.VMEM((CORES, *piece, side, layers, side, unit, LANES), BF16),
                pltpu.VMEM((2, kinds, layers, block, LANES), F32),
            ),
            in_specs=[hbm] * 12,
            out_specs=(vmem, vmem),
            scratch_shapes=[
                pltpu.VMEM((3, *piece, side, layers, unit, LANES), BF16),
                pltpu.VMEM((3, *piece, layers, unit, LANES), BF16),
                pltpu.VMEM((*piece, layers, unit, LANES), F32),
                pltpu.VMEM((*piece, layers, unit, LANES), BF16),
                pltpu.VMEM((kinds, layers, block, LANES), BF16),
                pltpu.VMEM((kinds, layers, block, LANES), F32),
                pltpu.VMEM((kinds, layers, block, LANES), F32),
                pltpu.VMEM((n, 1, LANES), F32),
            ],
            compiler_params=pltpu.CompilerParams(collective_id=0, has_side_effects=True, vmem_limit_bytes=33 << 20),
            name="exchange",
        )(*g, *w, *states)
        out = pl.pallas_call(
            functools.partial(write_kernel, side),
            out_shape=tuple(jax.ShapeDtypeStruct(a.shape, a.dtype) for a in (*w, *states)),
            in_specs=[vmem] * 2,
            out_specs=(hbm,) * 9,
            scratch_shapes=[dma((2,))],
            compiler_params=pltpu.CompilerParams(vmem_limit_bytes=1 << 20),
            name="write",
        )(*(pltpu.with_memory_space_constraint(a, pltpu.VMEM) for a in (whole, moments)))
        return tuple(untiled(o, a.shape) for o, a in zip(out, (*weights, *m, *v), strict=True))

    all_of, cut = P(None, None, None), P(None, "dp", None)
    return jax.shard_map(
        step,
        mesh=mesh,
        in_specs=(P(("rep", "dp"), None, None, None),) * 3 + (all_of,) * 3 + (cut,) * 6,
        out_specs=(P("rep", None, None),) * 3 + (P("rep", "dp", None),) * 6,
        check_vma=False,
    )
```
